32 devices in a mesh: dp: 4 (over y, x), expert: 8 (over z, core).
Axes of the slice: x: 2, y: 2, z: 4, core: 2. Of those that a mesh axis runs over, the one named last changes fastest.
Arguments:
- master: float32 [2, 32, 64, 2880], P(None, 'expert', 'dp'), may hold values from -6 to 6
- moment_one: float32 [2, 32, 64, 2880], P(None, 'expert', 'dp'), may hold values from -1.2 to 1.2
- moment_two: float32 [2, 32, 64, 2880], P(None, 'expert', 'dp'), may hold values from 0.0005 to 0.5
- gradient: bfloat16 [2, 32, 64, 2880], P(None, 'expert', 'dp'), may hold values from -150000 to 150000
- old_slot: int32 [2, 32], replicated, may hold values from 0 to 31, as said below
- new_slot: int32 [2, 32], replicated, may hold values from 0 to 31, as said below
Outputs:
- new_master: float32 [2, 32, 64, 2880], P(None, 'expert', 'dp')
- new_moment_one: float32 [2, 32, 64, 2880], P(None, 'expert', 'dp')
- new_moment_two: float32 [2, 32, 64, 2880], P(None, 'expert', 'dp')
The draws below stay inside these ranges and needn't reach their ends.
Inputs may be any that keep to these rules, and one draw needn't show every extreme that they name: `old_slot`: for each layer a permutation of 0 to 31; global slot s is held by index s // 4 of expert. `new_slot`: for each layer a permutation of 0 to 31; in each layer exactly 1 slot of each index of expert receives another expert than it held, and exactly 1 of the experts held by each index leaves its slot; all other experts keep their slot.
All inputs are finite; a program needn't handle non-finite values.
Results may differ from the reference program's by a relative error of at most 0.001.
Values sent between devices are 32-bit elements; how exact they have to be, the bound alone decides.
No kernel may reach another device: no remote copies, remote signals or barrier semaphores. Data moves between devices by JAX's collectives and lax.ppermute only.
A program may use at most 64 MiB of HBM per device.

```python
import math
import jax
import jax.numpy as jnp
from jax import lax

D = 2880
EXP_DEV = 4
EXPERTS = 32
RROWS = 64
LAYERS = 2
MOVE_DEV = 1


def placement_pair(key):
    base_key = jax.random.fold_in(key, 17)
    group_size = EXPERTS // EXP_DEV
    old_tables = []
    new_tables = []
    for layer_index in range(LAYERS):
        layer_key = jax.random.fold_in(base_key, layer_index)
        key_perm, key_pick, key_cycle = jax.random.split(layer_key, 3)
        old_layer = jax.random.permutation(key_perm, EXPERTS).astype(jnp.int32)
        scores = jax.random.randint(key_pick, (group_size, EXP_DEV), 0, 1 << 20, dtype=jnp.int32) * EXP_DEV
        scores = scores + lax.broadcasted_iota(jnp.int32, (group_size, EXP_DEV), 1)
        chosen = jnp.argsort(scores, axis=1)[:, :MOVE_DEV].astype(jnp.int32)
        chosen = (chosen + lax.broadcasted_iota(jnp.int32, chosen.shape, 0) * EXP_DEV).reshape(-1)
        cycle_order = jax.random.permutation(key_cycle, group_size * MOVE_DEV).astype(jnp.int32)
        ordered = chosen[cycle_order]
        destination = jnp.arange(EXPERTS, dtype=jnp.int32).at[ordered].set(jnp.roll(ordered, -1))
        old_tables.append(old_layer)
        new_tables.append(destination[old_layer].astype(jnp.int32))
    return (jnp.stack(old_tables), jnp.stack(new_tables))


def draw_old_slot(key, part):
    return placement_pair(key)[0]


def draw_new_slot(key, part):
    return placement_pair(key)[1]


def draw_gradient(key, part):
    key_noise = jax.random.fold_in(jax.random.fold_in(key, 29), 0)
    key_row = jax.random.fold_in(jax.random.fold_in(key, 29), 1)
    key_col = jax.random.fold_in(jax.random.fold_in(key, 29), 2)
    key_block = jax.random.fold_in(jax.random.fold_in(key, 29), 4)
    key_total = jax.random.fold_in(jax.random.fold_in(key, 29), 5)
    full_shape = (LAYERS, EXPERTS, RROWS, D)
    slot_place = lax.broadcasted_iota(jnp.float32, (1, EXPERTS, 1, 1), 1) / (EXPERTS - 1)
    block_scale = jnp.exp(jax.random.uniform(key_block, (LAYERS, EXPERTS, 1, 1), jnp.float32, 0.0, math.log(2.0)))
    total_scale = jnp.exp(jax.random.uniform(key_total, (), jnp.float32, 0.0, math.log(4.0)))
    slot_rise = 1.0 + 2.0 * slot_place
    noise = jax.random.normal(key_noise, full_shape, jnp.float32)
    row_scale = jnp.exp(jax.random.uniform(key_row, (LAYERS, EXPERTS, RROWS, 1), jnp.float32, 0.0, math.log(10.0)))
    col_scale = jnp.exp(jax.random.uniform(key_col, (LAYERS, 1, 1, D), jnp.float32, 0.0, math.log(10.0)))
    return (noise * row_scale * col_scale * slot_rise * block_scale * total_scale).astype(jnp.bfloat16)


def steps_of(own_key, extent, cuts, smallest, high):
    def one(dim, shards_of):
        heights = jax.random.uniform(jax.random.fold_in(jax.random.fold_in(own_key, 6), dim), (shards_of,), jnp.float32, smallest / len(cuts), high / len(cuts))
        return jnp.repeat(jnp.exp(heights), extent[dim] // shards_of).reshape((-1,) + (1,) * (len(extent) - dim - 1))

    gain = one(*cuts[0])
    for cut in cuts[1:]:
        gain = gain * one(*cut)
    return gain


def gaussian(stream_key, dims, scale, reach, cuts=(), kind=jnp.bfloat16):
    array = scale * jax.random.normal(stream_key, dims, jnp.float32)
    if cuts:
        array = array * steps_of(stream_key, dims, cuts, -0.22, 0.18)
    return jnp.clip(array, -reach, reach).astype(kind)


def setup_inputs(seed: int = 0) -> dict:
    key_of = jax.random.split(jax.random.key(seed), 7)
    return {
        "master": gaussian(key_of[0], (LAYERS, EXPERTS, RROWS, D), 1.0, 6.0, ((1, 8), (2, 4)), jnp.float32),
        "moment_one": gaussian(key_of[1], (LAYERS, EXPERTS, RROWS, D), 0.2, 1.2, ((1, 8), (2, 4)), jnp.float32),
        "moment_two": jnp.clip(jnp.exp(math.log(0.5) - 6.9077552 * jax.random.uniform(key_of[2], (LAYERS, EXPERTS, RROWS, D), jnp.float32) ** steps_of(key_of[2], (LAYERS, EXPERTS, RROWS, D), ((1, 8), (2, 4)), -0.2, 0.2)), 0.0005, 0.5),
        "gradient": draw_gradient(jax.random.fold_in(key_of[6], 71), 0),
        "old_slot": draw_old_slot(jax.random.fold_in(key_of[6], 71), 0),
        "new_slot": draw_new_slot(jax.random.fold_in(key_of[6], 71), 0),
    }


BETA_ONE = 0.9
BETA_TWO = 0.95
LEARN_RATE = 0.05
DECAY_RATE = 0.1
ADAM_EPS = 1e-08
CLIP_RMS = 2.0
FIRST_FIX = 1.0 - 0.9 ** 10
SECOND_FIX = 1.0 - 0.95 ** 10

def adam_update(master, moment_one, moment_two, gradient, clip_scale):
    scaled = gradient.astype(jnp.float32) * clip_scale
    first_moment = BETA_ONE * moment_one + (1.0 - BETA_ONE) * scaled
    second = BETA_TWO * moment_two + (1.0 - BETA_TWO) * scaled * scaled
    step_dir = first_moment / FIRST_FIX / (jnp.sqrt(second / SECOND_FIX) + ADAM_EPS)
    weights = master - LEARN_RATE * (step_dir + DECAY_RATE * master)
    return (weights, first_moment, second)

def clip_factor(square_sum, entry_count):
    return jnp.minimum(1.0, CLIP_RMS * math.sqrt(entry_count) / (jnp.sqrt(square_sum) + 1e-06))

def pick_rows(data, chosen):
    return jax.vmap(lambda layer_block, layer_pick: jnp.take(layer_block, layer_pick, axis=0))(data, chosen)

def reference(master, moment_one, moment_two, gradient, old_slot, new_slot):
    widened = gradient.astype(jnp.float32)
    square_sum = jnp.sum(widened * widened)
    clip_scale = clip_factor(square_sum, LAYERS * EXPERTS * RROWS * D)
    updated = adam_update(master, moment_one, moment_two, gradient, clip_scale)
    holder = jnp.argsort(new_slot, axis=1).astype(jnp.int32)
    source = jnp.take_along_axis(old_slot, holder, axis=1).astype(jnp.int32)
    return (pick_rows(updated[0], source), pick_rows(updated[1], source), pick_rows(updated[2], source))
```

```python
import functools
import math

import jax
import jax.numpy as jnp
from jax import lax
from jax.experimental import pallas as pl
from jax.experimental.pallas import tpu as pltpu
from jax.sharding import PartitionSpec as P

BETA_ONE = 0.9
BETA_TWO = 0.95
LEARN_RATE = 0.05
DECAY_RATE = 0.1
ADAM_EPS = 1e-08
CLIP_RMS = 2.0
FIRST_FIX = 1.0 - 0.9**10
SECOND_FIX = 1.0 - 0.95**10

LANES = 128
CORES = 2
EARLY = 0.5

ANY = pl.BlockSpec(memory_space=pl.ANY)
SMEM = pl.BlockSpec(memory_space=pltpu.SMEM)
VMEM = pl.BlockSpec(memory_space=pltpu.VMEM)


def up(n):
    return -(-n // LANES) * LANES


def moments(moment_one, moment_two, gradient, clip_scale):
    scaled = gradient * clip_scale
    first = BETA_ONE * moment_one + (1.0 - BETA_ONE) * scaled
    second = BETA_TWO * moment_two + (1.0 - BETA_TWO) * scaled * scaled
    return first, second


def new_weights(master, first, second):
    step_dir = first / FIRST_FIX / (jnp.sqrt(second / SECOND_FIX) + ADAM_EPS)
    return master - LEARN_RATE * (step_dir + DECAY_RATE * master)


class Sizes:
    def __init__(self, shape, group, dp):
        self.layers, self.slots, self.rows, self.cols = shape
        self.group = group
        self.devices = group * dp
        self.chips = group // CORES
        self.piece = self.layers * self.rows // self.chips
        self.per_layer = self.rows // self.piece
        early = up(int(self.cols * EARLY)) - LANES
        self.early = early
        self.late = self.cols - early
        self.lat = up(self.late)
        self.full = up(self.cols)
        self.w_one = self.full + 3 * early
        self.w_two = self.full + 2 * early
        self.w_late = 2 * self.lat


def peer(i, x, n):
    return i ^ x if n & (n - 1) == 0 else (i + x) % n


def source_peer(i, x, n):
    return i ^ x if n & (n - 1) == 0 else lax.rem(i - x + n, n)


def dyn_peer(i, x, n):
    return i ^ x if n & (n - 1) == 0 else lax.rem(i + x, n)


def prep_kernel(sz, me_ref, old_ref, new_ref, master, mone, mtwo, grad, *rest):
    c = sz.chips
    pieces = rest[:c]
    late_raw, total, plan = rest[c : c + 3]
    mv, m1v, m2v, gv, st, sem_g, sem = rest[c + 3 :]
    for i in range(sz.layers):
        pltpu.make_async_copy(grad.at[i], gv.at[i], sem_g.at[i]).start()
    me = me_ref[0]
    chip = lax.div(me, CORES)
    n_slots = sz.layers * sz.group

    for i in range(sz.layers):
        def note(e, carry):
            o = old_ref[i, e]
            n = new_ref[i, e]
            place = jnp.where(o != n, i * sz.group + lax.div(n, sz.slots), n_slots)
            plan[0, place] = lax.div(o, sz.slots)
            plan[1, place] = lax.rem(n, sz.slots)
            return carry

        lax.fori_loop(0, old_ref.shape[1], note, 0)
    copies = []
    for i in range(sz.layers):
        slot = plan[1, i * sz.group + me]
        for a, (src, dst) in enumerate(((master, mv), (mone, m1v), (mtwo, m2v))):
            cp = pltpu.make_async_copy(src.at[i, slot], dst.at[i], sem.at[i, a])
            cp.start()
            copies.append(cp)
    acc = jnp.zeros((sz.rows, sz.cols), jnp.float32)
    for i in range(sz.layers):
        pltpu.make_async_copy(grad.at[i], gv.at[i], sem_g.at[i]).wait()
        for s in range(sz.slots):
            x = gv[i, s].astype(jnp.float32)
            acc = acc + x * x
    total[...] = jnp.broadcast_to(jnp.sum(acc), total.shape)
    for cp in copies:
        cp.wait()
    for i in range(sz.layers):
        slot = plan[1, i * sz.group + me]
        g = gv[i, slot].astype(jnp.float32)
        for q in range(sz.per_layer):
            k = i * sz.per_layer + q
            r = slice(q * sz.piece, (q + 1) * sz.piece)
            st[0, k] = mv[i, r, :]
            st[1, k] = m1v[i, r, :]
            st[2, k] = m2v[i, r, :]
            st[3, k] = g[r, :]
    for x in range(c):
        k = dyn_peer(chip, x, c)
        pieces[x][:, : sz.cols] = st[0, k]
        for a in range(3):
            lo = sz.full + a * sz.early
            pieces[x][:, lo : lo + sz.early] = st[a + 1, k, :, : sz.early]
            late_raw[a, x] = st[a + 1, k, :, sz.early :]


def prep(sz, me, old_slot, new_slot, master, mone, mtwo, grad):
    f32 = jnp.float32
    slot = (sz.layers, sz.rows, sz.cols)
    outs = [jax.ShapeDtypeStruct((sz.piece, sz.w_one), f32)] * sz.chips + [
        jax.ShapeDtypeStruct((3, sz.chips, sz.piece, sz.late), f32),
        jax.ShapeDtypeStruct((sz.devices, LANES), f32),
        jax.ShapeDtypeStruct((2, sz.layers * sz.group + 1), jnp.int32),
    ]
    return pl.pallas_call(
        functools.partial(prep_kernel, sz),
        in_specs=[SMEM, SMEM, SMEM, ANY, ANY, ANY, ANY],
        out_specs=[VMEM] * (sz.chips + 2) + [SMEM],
        out_shape=outs,
        scratch_shapes=[
            pltpu.VMEM(slot, f32),
            pltpu.VMEM(slot, f32),
            pltpu.VMEM(slot, f32),
            pltpu.VMEM(grad.shape, grad.dtype),
            pltpu.VMEM((4, sz.chips, sz.piece, sz.cols), f32),
            pltpu.SemaphoreType.DMA((sz.layers,)),
            pltpu.SemaphoreType.DMA((sz.layers, 3)),
        ],
        name="prep",
    )(me, old_slot, new_slot, master, mone, mtwo, grad)


def scale_kernel(sz, total, raw, clip, *late):
    entries = sz.layers * sz.slots * sz.rows * sz.cols * sz.devices
    square_sum = jnp.sum(total[:, 0:1])
    root = jnp.sqrt(jnp.full((1, LANES), square_sum, jnp.float32))
    scale = jnp.minimum(1.0, CLIP_RMS * math.sqrt(entries) / (root + 1e-06))
    clip[...] = scale
    for x in range(sz.chips):
        first, second = moments(raw[0, x], raw[1, x], raw[2, x], scale[:, 0:1])
        late[x][:, : sz.late] = first
        late[x][:, sz.lat : sz.lat + sz.late] = second


def scale_and_late(sz, total, raw):
    f32 = jnp.float32
    return pl.pallas_call(
        functools.partial(scale_kernel, sz),
        in_specs=[VMEM, VMEM],
        out_specs=[VMEM] * (sz.chips + 1),
        out_shape=[jax.ShapeDtypeStruct((1, LANES), f32)]
        + [jax.ShapeDtypeStruct((sz.piece, sz.w_late), f32)] * sz.chips,
        name="scale_late",
    )(total, raw)


def pick_kernel(sz, early, me_ref, plan, *rest):
    c = sz.chips
    if early:
        clip, rest = rest[0], rest[1:]
    refs = rest[: 2 * c]
    outs = rest[2 * c : 3 * c]
    if early:
        hold, sem = rest[3 * c :]
        spots = [hold.at[x] for x in range(c)]
    else:
        sem = rest[3 * c]
        spots = outs
    me = me_ref[0]
    chip = lax.div(me, CORES)
    core = lax.rem(me, CORES)
    layer = lax.div(chip, sz.per_layer)
    for x in range(c):
        target = dyn_peer(chip, x, c) * CORES + core
        sender = plan[0, layer * sz.group + target]
        away = source_peer(chip, 0, c)
        from_chip = lax.div(sender, CORES)
        shift = from_chip ^ chip if c & (c - 1) == 0 else lax.rem(chip - from_chip + c, c)
        choice = shift + jnp.where(lax.rem(sender, CORES) == core, 0, c)
        for q in range(2 * c):
            @pl.when(choice == q)
            def _():
                pltpu.make_async_copy(refs[q], spots[x], sem.at[x]).start()
    for x in range(c):
        pltpu.make_async_copy(refs[0], spots[x], sem.at[x]).wait()
        if early:
            scale = clip[:, 0:1]
            at = [sz.full + a * sz.early for a in range(3)]
            parts = [hold[x, :, lo : lo + sz.early] for lo in at]
            first, second = moments(*parts, scale)
            outs[x][:, : sz.full] = hold[x, :, : sz.full]
            outs[x][:, at[0] : at[0] + sz.early] = first
            outs[x][:, at[1] : at[1] + sz.early] = second


def pick(sz, early, me, plan, clip, own, other):
    f32 = jnp.float32
    c = sz.chips
    width = sz.w_two if early else sz.w_late
    scratch = [pltpu.VMEM((c, sz.piece, sz.w_one), f32)] if early else []
    return pl.pallas_call(
        functools.partial(pick_kernel, sz, early),
        in_specs=[SMEM, SMEM] + ([VMEM] if early else []) + [ANY] * (2 * c),
        out_specs=[VMEM if early else ANY] * c,
        out_shape=[jax.ShapeDtypeStruct((sz.piece, width), f32)] * c,
        scratch_shapes=scratch + [pltpu.SemaphoreType.DMA((c,))],
        name="pick_early" if early else "pick_late",
    )(me, plan, *([clip] if early else []), *own, *other)


def land_kernel(sz, me_ref, plan, *rest):
    c = sz.chips
    early, late = rest[:c], rest[c : 2 * c]
    outs = rest[2 * c + 3 : 2 * c + 6]
    st, full, sem = rest[2 * c + 6 :]
    me = me_ref[0]
    chip = lax.div(me, CORES)
    e, f = sz.early, sz.full
    for x in range(c):
        k = dyn_peer(chip, x, c) if c & (c - 1) == 0 else lax.rem(chip - x + c, c)
        a, b = early[x], late[x]
        first, second = a[:, f : f + e], a[:, f + e : f + 2 * e]
        st[0, k, :, :e] = new_weights(a[:, :e], first, second)
        st[1, k, :, :e] = first
        st[2, k, :, :e] = second
        first, second = b[:, : sz.late], b[:, sz.lat : sz.lat + sz.late]
        st[0, k, :, e:] = new_weights(a[:, e : sz.cols], first, second)
        st[1, k, :, e:] = first
        st[2, k, :, e:] = second
    copies = []
    for i in range(sz.layers):
        slot = plan[1, i * sz.group + me]
        for a in range(3):
            for q in range(sz.per_layer):
                r = slice(q * sz.piece, (q + 1) * sz.piece)
                full[a, i, r, :] = st[a, i * sz.per_layer + q]
            cp = pltpu.make_async_copy(full.at[a, i], outs[a].at[i, slot], sem.at[a, i])
            cp.start()
            copies.append(cp)
    for cp in copies:
        cp.wait()


def land(sz, me, plan, early, late, outs):
    f32 = jnp.float32
    c = sz.chips
    return pl.pallas_call(
        functools.partial(land_kernel, sz),
        in_specs=[SMEM, SMEM] + [VMEM] * (2 * c) + [ANY] * 3,
        out_specs=[ANY] * 3,
        out_shape=[jax.ShapeDtypeStruct(o.shape, o.dtype) for o in outs],
        scratch_shapes=[
            pltpu.VMEM((3, c, sz.piece, sz.cols), f32),
            pltpu.VMEM((3, sz.layers, sz.rows, sz.cols), f32),
            pltpu.SemaphoreType.DMA((3, sz.layers)),
        ],
        input_output_aliases={2 + 2 * c + a: a for a in range(3)},
        name="land",
    )(me, plan, *early, *late, *outs)


def spread(sz, arrays):
    c = sz.chips
    got = [arrays[0]]
    for x in range(1, c):
        pairs = [
            (i * CORES + k, peer(i, x, c) * CORES + k) for i in range(c) for k in range(CORES)
        ]
        got.append(lax.ppermute(arrays[x], "expert", pairs))
    return got


def swap(sz, arrays):
    pairs = [(i, i ^ 1) for i in range(sz.group)]
    return [lax.ppermute(a, "expert", pairs) for a in arrays]


def shards(master, moment_one, moment_two, gradient, old_slot, new_slot):
    sz = Sizes(master.shape, lax.axis_size("expert"), lax.axis_size("dp"))
    me = lax.axis_index("expert").reshape(1)
    c = sz.chips
    got = prep(sz, me, old_slot, new_slot, master, moment_one, moment_two, gradient)
    pieces, raw, partial, plan = got[:c], got[c], got[c + 1], got[c + 2]
    held = spread(sz, pieces)
    sums = lax.all_to_all(partial, ("dp", "expert"), 0, 0, tiled=True)
    clip, *late = scale_and_late(sz, sums, raw)
    late_held = spread(sz, late)
    other = swap(sz, held)
    early_out = pick(sz, True, me, plan, clip, held, other)
    early_in = spread(sz, early_out)
    late_other = swap(sz, late_held)
    late_out = pick(sz, False, me, plan, None, late_held, late_other)
    late_in = spread(sz, late_out)
    scale = clip[0, 0]
    first, second = moments(moment_one, moment_two, gradient.astype(jnp.float32), scale)
    weights = new_weights(master, first, second)
    return tuple(land(sz, me, plan, early_in, late_in, (weights, first, second)))


def solution(mesh):
    spec = P(None, "expert", "dp", None)
    return jax.shard_map(
        shards,
        mesh=mesh,
        in_specs=(spec, spec, spec, spec, P(), P()),
        out_specs=(spec, spec, spec),
        check_vma=False,
    )
```

```python
import functools
import math

import jax
import jax.numpy as jnp
from jax import lax
from jax.experimental import pallas as pl
from jax.experimental.pallas import tpu as pltpu
from jax.sharding import PartitionSpec as P


BETA_ONE = 0.9
BETA_TWO = 0.95
LEARN_RATE = 0.05
DECAY_RATE = 0.1
ADAM_EPS = 1e-08
CLIP_RMS = 2.0
FIRST_FIX = 1.0 - 0.9**10
SECOND_FIX = 1.0 - 0.95**10

LANES = 128
CORES = 2
EARLY = 0.5

ANY = pl.BlockSpec(memory_space=pl.ANY)
SMEM = pl.BlockSpec(memory_space=pltpu.SMEM)
VMEM = pl.BlockSpec(memory_space=pltpu.VMEM)


def out(*shape, dtype=jnp.float32):
    return pltpu.VMEM(shape, dtype)


def near(arrays):
    return [pltpu.with_memory_space_constraint(a, pltpu.VMEM) for a in arrays]


def up(n):
    return -(-n // LANES) * LANES


def moments(moment_one, moment_two, gradient, clip_scale):
    scaled = gradient * clip_scale
    first = BETA_ONE * moment_one + (1.0 - BETA_ONE) * scaled
    second = BETA_TWO * moment_two + (1.0 - BETA_TWO) * scaled * scaled
    return first, second


def new_weights(master, first, second):
    step_dir = first / FIRST_FIX / (jnp.sqrt(second / SECOND_FIX) + ADAM_EPS)
    return master - LEARN_RATE * (step_dir + DECAY_RATE * master)


class Sizes:
    def __init__(self, shape, group, dp):
        self.layers, self.slots, self.rows, self.cols = shape
        self.group = group
        self.devices = group * dp
        self.chips = group // CORES
        self.piece = self.layers * self.rows // self.chips
        self.per_layer = self.rows // self.piece
        early = up(int(self.cols * EARLY)) - LANES
        self.early = early
        self.late = self.cols - early
        self.lat = up(self.late)
        self.full = up(self.cols)
        self.w_one = self.full + 3 * early
        self.w_two = self.full + 2 * early
        self.w_late = 2 * self.lat


def peer(i, x, n):
    return i ^ x if n & (n - 1) == 0 else (i + x) % n


def dyn_peer(i, x, n):
    return i ^ x if n & (n - 1) == 0 else lax.rem(i + x, n)


def prep_kernel(sz, me_ref, old_ref, new_ref, master, mone, mtwo, grad, *rest):
    c = sz.chips
    pieces = rest[:c]
    late_raw, plan = rest[c : c + 2]
    mv, m1v, m2v, gv, st, sem = rest[c + 2 :]
    me = me_ref[0]
    chip = lax.div(me, CORES)
    n_slots = sz.layers * sz.group

    for i in range(sz.layers):
        def note(e, carry):
            o = old_ref[i, e]
            n = new_ref[i, e]
            place = jnp.where(o != n, i * sz.group + lax.div(n, sz.slots), n_slots)
            plan[0, place] = lax.div(o, sz.slots)
            plan[1, place] = lax.rem(n, sz.slots)
            return carry

        lax.fori_loop(0, old_ref.shape[1], note, 0, unroll=8)
        slot = plan[1, i * sz.group + me]
        for a, (src, dst) in enumerate(((master, mv), (mone, m1v), (mtwo, m2v), (grad, gv))):
            pltpu.make_async_copy(src.at[i, slot], dst.at[i], sem.at[i, a]).start()
    for i in range(sz.layers):
        for a, (src, dst) in enumerate(((master, mv), (mone, m1v), (mtwo, m2v), (grad, gv))):
            pltpu.make_async_copy(src.at[i, 0], dst.at[i], sem.at[i, a]).wait()
        g = gv[i].astype(jnp.float32)
        for q in range(sz.per_layer):
            k = i * sz.per_layer + q
            r = slice(q * sz.piece, (q + 1) * sz.piece)
            st[0, k] = mv[i, r, :]
            st[1, k] = m1v[i, r, :]
            st[2, k] = m2v[i, r, :]
            st[3, k] = g[r, :]
    for x in range(c):
        k = dyn_peer(chip, x, c)
        pieces[x][:, : sz.cols] = st[0, k]
        for a in range(3):
            lo = sz.full + a * sz.early
            pieces[x][:, lo : lo + sz.early] = st[a + 1, k, :, : sz.early]
            late_raw[a, x] = st[a + 1, k, :, sz.early :]


def prep(sz, me, old_slot, new_slot, master, mone, mtwo, grad):
    f32 = jnp.float32
    slot = (sz.layers, sz.rows, sz.cols)
    outs = [out(sz.piece, sz.w_one)] * sz.chips + [
        out(3, sz.chips, sz.piece, sz.late),
        jax.ShapeDtypeStruct((2, sz.layers * sz.group + 1), jnp.int32),
    ]
    return pl.pallas_call(
        functools.partial(prep_kernel, sz),
        in_specs=[SMEM, SMEM, SMEM, ANY, ANY, ANY, ANY],
        out_specs=[VMEM] * (sz.chips + 1) + [SMEM],
        out_shape=outs,
        scratch_shapes=[
            pltpu.VMEM(slot, f32),
            pltpu.VMEM(slot, f32),
            pltpu.VMEM(slot, f32),
            pltpu.VMEM(slot, grad.dtype),
            pltpu.VMEM((4, sz.chips, sz.piece, sz.cols), f32),
            pltpu.SemaphoreType.DMA((sz.layers, 4)),
        ],
        name="prep",
    )(me, old_slot, new_slot, master, mone, mtwo, grad)


def square_kernel(sz, grad, total, gv, sem):
    copies = [pltpu.make_async_copy(grad.at[i], gv.at[i], sem.at[i]) for i in range(sz.layers)]
    for cp in copies:
        cp.start()
    acc = jnp.zeros((sz.rows, sz.cols), jnp.float32)
    for i in range(sz.layers):
        copies[i].wait()
        for s in range(sz.slots):
            x = gv[i, s].astype(jnp.float32)
            acc = acc + x * x
    total[...] = jnp.broadcast_to(jnp.sum(acc), total.shape)


def squares(sz, grad):
    return pl.pallas_call(
        functools.partial(square_kernel, sz),
        in_specs=[ANY],
        out_specs=VMEM,
        out_shape=out(sz.devices, LANES),
        scratch_shapes=[
            pltpu.VMEM(grad.shape, grad.dtype),
            pltpu.SemaphoreType.DMA((sz.layers,)),
        ],
        name="squares",
    )(grad)


def scale_kernel(sz, total, raw, clip, *late):
    entries = sz.layers * sz.slots * sz.rows * sz.cols * sz.devices
    square_sum = jnp.sum(total[:, 0:1])
    root = jnp.sqrt(jnp.full((1, LANES), square_sum, jnp.float32))
    scale = jnp.minimum(1.0, CLIP_RMS * math.sqrt(entries) / (root + 1e-06))
    clip[...] = scale
    for x in range(sz.chips):
        first, second = moments(raw[0, x], raw[1, x], raw[2, x], scale[:, 0:1])
        late[x][:, : sz.late] = first
        late[x][:, sz.lat : sz.lat + sz.late] = second


def scale_and_late(sz, total, raw):
    return pl.pallas_call(
        functools.partial(scale_kernel, sz),
        in_specs=[VMEM, VMEM],
        out_specs=[VMEM] * (sz.chips + 1),
        out_shape=[out(1, LANES)] + [out(sz.piece, sz.w_late)] * sz.chips,
        name="scale_late",
    )(*near((total, raw)))


def pick_kernel(sz, early, me_ref, plan, *rest):
    c = sz.chips
    if early:
        clip, rest = rest[0], rest[1:]
    refs = rest[: 2 * c]
    outs = rest[2 * c : 3 * c]
    me = me_ref[0]
    chip = lax.div(me, CORES)
    core = lax.rem(me, CORES)
    layer = lax.div(chip, sz.per_layer)
    for x in range(c):
        target = dyn_peer(chip, x, c) * CORES + core
        sender = plan[0, layer * sz.group + target]
        from_chip = lax.div(sender, CORES)
        shift = from_chip ^ chip if c & (c - 1) == 0 else lax.rem(chip - from_chip + c, c)
        choice = shift + jnp.where(lax.rem(sender, CORES) == core, 0, c)
        for q in range(2 * c):
            @pl.when(choice == q)
            def _():
                if not early:
                    outs[x][...] = refs[q][...]
                    return
                at = [sz.full + a * sz.early for a in range(3)]
                parts = [refs[q][:, lo : lo + sz.early] for lo in at]
                first, second = moments(*parts, clip[:, 0:1])
                outs[x][:, : sz.full] = refs[q][:, : sz.full]
                outs[x][:, at[0] : at[0] + sz.early] = first
                outs[x][:, at[1] : at[1] + sz.early] = second


def pick(sz, early, me, plan, clip, own, other):
    c = sz.chips
    width = sz.w_two if early else sz.w_late
    vectors = ([clip] if early else []) + own + other
    return pl.pallas_call(
        functools.partial(pick_kernel, sz, early),
        in_specs=[SMEM, SMEM] + [VMEM] * len(vectors),
        out_specs=[VMEM] * c,
        out_shape=[out(sz.piece, width)] * c,
        name="pick_early" if early else "pick_late",
    )(me, plan, *vectors)


def land_kernel(sz, me_ref, plan, *rest):
    c = sz.chips
    early, late = rest[:c], rest[c : 2 * c]
    outs = rest[2 * c + 3 : 2 * c + 6]
    st, full, sem = rest[2 * c + 6 :]
    me = me_ref[0]
    chip = lax.div(me, CORES)
    e, f = sz.early, sz.full
    for x in range(c):
        k = dyn_peer(chip, x, c) if c & (c - 1) == 0 else lax.rem(chip - x + c, c)
        a, b = early[x], late[x]
        first, second = a[:, f : f + e], a[:, f + e : f + 2 * e]
        st[0, k, :, :e] = new_weights(a[:, :e], first, second)
        st[1, k, :, :e] = first
        st[2, k, :, :e] = second
        first, second = b[:, : sz.late], b[:, sz.lat : sz.lat + sz.late]
        st[0, k, :, e:] = new_weights(a[:, e : sz.cols], first, second)
        st[1, k, :, e:] = first
        st[2, k, :, e:] = second
    copies = []
    for i in range(sz.layers):
        slot = plan[1, i * sz.group + me]
        for a in range(3):
            for q in range(sz.per_layer):
                r = slice(q * sz.piece, (q + 1) * sz.piece)
                full[a, i, r, :] = st[a, i * sz.per_layer + q]
            cp = pltpu.make_async_copy(full.at[a, i], outs[a].at[i, slot], sem.at[a, i])
            cp.start()
            copies.append(cp)
    for cp in copies:
        cp.wait()


def land(sz, me, plan, early, late, outs):
    f32 = jnp.float32
    c = sz.chips
    return pl.pallas_call(
        functools.partial(land_kernel, sz),
        in_specs=[SMEM, SMEM] + [VMEM] * (2 * c) + [ANY] * 3,
        out_specs=[ANY] * 3,
        out_shape=[jax.ShapeDtypeStruct(o.shape, o.dtype) for o in outs],
        scratch_shapes=[
            pltpu.VMEM((3, c, sz.piece, sz.cols), f32),
            pltpu.VMEM((3, sz.layers, sz.rows, sz.cols), f32),
            pltpu.SemaphoreType.DMA((3, sz.layers)),
        ],
        input_output_aliases={2 + 2 * c + a: a for a in range(3)},
        name="land",
    )(me, plan, *early, *late, *outs)


def spread(sz, arrays):
    c = sz.chips
    got = [arrays[0]]
    for x in range(1, c):
        pairs = [
            (i * CORES + k, peer(i, x, c) * CORES + k) for i in range(c) for k in range(CORES)
        ]
        got.append(lax.ppermute(arrays[x], "expert", pairs))
    return got[:1] + near(got[1:])


def swap(sz, arrays):
    pairs = [(i, i ^ 1) for i in range(sz.group)]
    return near([lax.ppermute(a, "expert", pairs) for a in arrays])


def shards(master, moment_one, moment_two, gradient, old_slot, new_slot):
    sz = Sizes(master.shape, lax.axis_size("expert"), lax.axis_size("dp"))
    me = lax.axis_index("expert").reshape(1)
    c = sz.chips
    got = prep(sz, me, old_slot, new_slot, master, moment_one, moment_two, gradient)
    pieces, raw, plan = list(got[:c]), got[c], got[c + 1]
    held = spread(sz, pieces)
    partial = squares(sz, gradient)
    sums = lax.all_to_all(partial, ("dp", "expert"), 0, 0, tiled=True)
    clip, *late = scale_and_late(sz, sums, raw)
    late_held = spread(sz, late)
    other = swap(sz, held)
    early_out = pick(sz, True, me, plan, clip, held, other)
    early_in = spread(sz, list(early_out))
    late_other = swap(sz, late_held)
    late_out = pick(sz, False, me, plan, None, late_held, late_other)
    late_in = spread(sz, list(late_out))
    scale = clip[0, 0]
    wide = gradient.astype(jnp.float32)
    first, second = moments(moment_one, moment_two, wide, scale)
    weights = new_weights(master, first, second)
    return tuple(land(sz, me, plan, early_in, late_in, (weights, first, second)))


def solution(mesh):
    spec = P(None, "expert", "dp", None)
    return jax.shard_map(
        shards,
        mesh=mesh,
        in_specs=(spec, spec, spec, spec, P(), P()),
        out_specs=(spec, spec, spec),
        check_vma=False,
    )
```

```python
import functools
import math

import jax
import jax.numpy as jnp
from jax import lax
from jax.experimental import pallas as pl
from jax.experimental.pallas import tpu as pltpu
from jax.sharding import PartitionSpec as P


BETA_ONE = 0.9
BETA_TWO = 0.95
LEARN_RATE = 0.05
DECAY_RATE = 0.1
ADAM_EPS = 1e-08
CLIP_RMS = 2.0
FIRST_FIX = 1.0 - 0.9**10
SECOND_FIX = 1.0 - 0.95**10

LANES = 128
CORES = 2
EARLY = 0.5

ANY = pl.BlockSpec(memory_space=pl.ANY)
SMEM = pl.BlockSpec(memory_space=pltpu.SMEM)
VMEM = pl.BlockSpec(memory_space=pltpu.VMEM)


def out(*shape, dtype=jnp.float32):
    return pltpu.VMEM(shape, dtype)


def near(arrays):
    return [pltpu.with_memory_space_constraint(a, pltpu.VMEM) for a in arrays]


def up(n):
    return -(-n // LANES) * LANES


def moments(moment_one, moment_two, gradient, clip_scale):
    scaled = gradient * clip_scale
    first = BETA_ONE * moment_one + (1.0 - BETA_ONE) * scaled
    second = BETA_TWO * moment_two + (1.0 - BETA_TWO) * scaled * scaled
    return first, second


def new_weights(master, first, second):
    step_dir = first / FIRST_FIX / (jnp.sqrt(second / SECOND_FIX) + ADAM_EPS)
    return master - LEARN_RATE * (step_dir + DECAY_RATE * master)


class Sizes:
    def __init__(self, shape, group, dp):
        self.layers, self.slots, self.rows, self.cols = shape
        self.group = group
        self.devices = group * dp
        self.chips = group // CORES
        self.piece = self.layers * self.rows // self.chips
        self.per_layer = self.rows // self.piece
        early = up(int(self.cols * EARLY)) - LANES
        self.early = early
        self.late = self.cols - early
        self.lat = up(self.late)
        self.full = up(self.cols)
        self.groups = ((self.full, 0, early, early), (0, early, self.late, self.lat))


def width(group, parts):
    head, _, _, stride = group
    return head + parts * stride


def peer(i, x, n):
    return i ^ x if n & (n - 1) == 0 else (i + x) % n


def dyn_peer(i, x, n):
    return i ^ x if n & (n - 1) == 0 else lax.rem(i + x, n)


def prep_kernel(sz, me_ref, old_ref, new_ref, master, mone, mtwo, grad, *rest):
    c = sz.chips
    pieces = rest[:c], rest[c : 2 * c]
    plan, mv, m1v, m2v, gv, st, sem = rest[2 * c :]
    me = me_ref[0]
    chip = lax.div(me, CORES)
    n_slots = sz.layers * sz.group

    for i in range(sz.layers):
        def note(e, carry):
            o = old_ref[i, e]
            n = new_ref[i, e]
            place = jnp.where(o != n, i * sz.group + lax.div(n, sz.slots), n_slots)
            plan[0, place] = lax.div(o, sz.slots)
            plan[1, place] = lax.rem(n, sz.slots)
            return carry

        lax.fori_loop(0, old_ref.shape[1], note, 0, unroll=8)
        slot = plan[1, i * sz.group + me]
        for a, (src, dst) in enumerate(((master, mv), (mone, m1v), (mtwo, m2v), (grad, gv))):
            pltpu.make_async_copy(src.at[i, slot], dst.at[i], sem.at[i, a]).start()
    for i in range(sz.layers):
        for a, (src, dst) in enumerate(((master, mv), (mone, m1v), (mtwo, m2v), (grad, gv))):
            pltpu.make_async_copy(src.at[i, 0], dst.at[i], sem.at[i, a]).wait()
        g = gv[i].astype(jnp.float32)
        for q in range(sz.per_layer):
            k = i * sz.per_layer + q
            r = slice(q * sz.piece, (q + 1) * sz.piece)
            st[0, k] = mv[i, r, :]
            st[1, k] = m1v[i, r, :]
            st[2, k] = m2v[i, r, :]
            st[3, k] = g[r, :]
    for x in range(c):
        k = dyn_peer(chip, x, c)
        pieces[0][x][:, : sz.cols] = st[0, k]
        for refs, (head, start, size, stride) in zip(pieces, sz.groups):
            for a in range(3):
                lo = head + a * stride
                refs[x][:, lo : lo + size] = st[a + 1, k, :, start : start + size]


def prep(sz, me, old_slot, new_slot, master, mone, mtwo, grad):
    f32 = jnp.float32
    slot = (sz.layers, sz.rows, sz.cols)
    outs = [out(sz.piece, width(g, 3)) for g in sz.groups for _ in range(sz.chips)]
    outs.append(jax.ShapeDtypeStruct((2, sz.layers * sz.group + 1), jnp.int32))
    return pl.pallas_call(
        functools.partial(prep_kernel, sz),
        in_specs=[SMEM, SMEM, SMEM, ANY, ANY, ANY, ANY],
        out_specs=[VMEM] * (2 * sz.chips) + [SMEM],
        out_shape=outs,
        scratch_shapes=[
            pltpu.VMEM(slot, f32),
            pltpu.VMEM(slot, f32),
            pltpu.VMEM(slot, f32),
            pltpu.VMEM(slot, grad.dtype),
            pltpu.VMEM((4, sz.chips, sz.piece, sz.cols), f32),
            pltpu.SemaphoreType.DMA((sz.layers, 4)),
        ],
        name="prep",
    )(me, old_slot, new_slot, master, mone, mtwo, grad)


def square_kernel(sz, grad, total, gv, sem):
    copies = [pltpu.make_async_copy(grad.at[i], gv.at[i], sem.at[i]) for i in range(sz.layers)]
    for cp in copies:
        cp.start()
    acc = jnp.zeros((sz.rows, sz.cols), jnp.float32)
    for i in range(sz.layers):
        copies[i].wait()
        for s in range(sz.slots):
            x = gv[i, s].astype(jnp.float32)
            acc = acc + x * x
    total[...] = jnp.broadcast_to(jnp.sum(acc), total.shape)


def squares(sz, grad):
    return pl.pallas_call(
        functools.partial(square_kernel, sz),
        in_specs=[ANY],
        out_specs=VMEM,
        out_shape=out(1, LANES),
        scratch_shapes=[
            pltpu.VMEM(grad.shape, grad.dtype),
            pltpu.SemaphoreType.DMA((sz.layers,)),
        ],
        name="squares",
    )(grad)


def scale_kernel(sz, *refs):
    entries = sz.layers * sz.slots * sz.rows * sz.cols * sz.devices
    square_sum = refs[0][...]
    for part in refs[1:-1]:
        square_sum = square_sum + part[...]
    refs[-1][...] = jnp.minimum(
        1.0, CLIP_RMS * math.sqrt(entries) / (jnp.sqrt(square_sum) + 1e-06)
    )


def clip_scale(sz, parts):
    return pl.pallas_call(
        functools.partial(scale_kernel, sz),
        in_specs=[VMEM] * len(parts),
        out_specs=VMEM,
        out_shape=out(1, LANES),
        name="clip_scale",
    )(*parts)


def pick_kernel(sz, group, me_ref, plan, clip, *rest):
    c = sz.chips
    refs = rest[: 2 * c]
    outs = rest[2 * c : 3 * c]
    head, _, size, stride = group
    at = [head + a * stride for a in range(3)]
    me = me_ref[0]
    chip = lax.div(me, CORES)
    core = lax.rem(me, CORES)
    layer = lax.div(chip, sz.per_layer)
    for x in range(c):
        target = dyn_peer(chip, x, c) * CORES + core
        sender = plan[0, layer * sz.group + target]
        from_chip = lax.div(sender, CORES)
        shift = from_chip ^ chip if c & (c - 1) == 0 else lax.rem(chip - from_chip + c, c)
        choice = shift + jnp.where(lax.rem(sender, CORES) == core, 0, c)
        for q in range(2 * c):
            @pl.when(choice == q)
            def _():
                parts = [refs[q][:, lo : lo + size] for lo in at]
                first, second = moments(*parts, clip[:, 0:1])
                if head:
                    outs[x][:, :head] = refs[q][:, :head]
                outs[x][:, at[0] : at[0] + size] = first
                outs[x][:, at[1] : at[1] + size] = second


def pick(sz, which, me, plan, clip, own, other):
    c = sz.chips
    group = sz.groups[which]
    return pl.pallas_call(
        functools.partial(pick_kernel, sz, group),
        in_specs=[SMEM, SMEM] + [VMEM] * (2 * c + 1),
        out_specs=[VMEM] * c,
        out_shape=[out(sz.piece, width(group, 2))] * c,
        name="pick",
    )(me, plan, clip, *own, *other)


def land_kernel(sz, me_ref, plan, *rest):
    c = sz.chips
    early, late = rest[:c], rest[c : 2 * c]
    outs = rest[2 * c + 3 : 2 * c + 6]
    st, full, sem = rest[2 * c + 6 :]
    me = me_ref[0]
    chip = lax.div(me, CORES)
    e, f = sz.early, sz.full
    for x in range(c):
        k = dyn_peer(chip, x, c) if c & (c - 1) == 0 else lax.rem(chip - x + c, c)
        a, b = early[x], late[x]
        first, second = a[:, f : f + e], a[:, f + e : f + 2 * e]
        st[0, k, :, :e] = new_weights(a[:, :e], first, second)
        st[1, k, :, :e] = first
        st[2, k, :, :e] = second
        first, second = b[:, : sz.late], b[:, sz.lat : sz.lat + sz.late]
        st[0, k, :, e:] = new_weights(a[:, e : sz.cols], first, second)
        st[1, k, :, e:] = first
        st[2, k, :, e:] = second
    copies = []
    for i in range(sz.layers):
        slot = plan[1, i * sz.group + me]
        for a in range(3):
            for q in range(sz.per_layer):
                r = slice(q * sz.piece, (q + 1) * sz.piece)
                full[a, i, r, :] = st[a, i * sz.per_layer + q]
            cp = pltpu.make_async_copy(full.at[a, i], outs[a].at[i, slot], sem.at[a, i])
            cp.start()
            copies.append(cp)
    for cp in copies:
        cp.wait()


def land(sz, me, plan, early, late, outs):
    f32 = jnp.float32
    c = sz.chips
    return pl.pallas_call(
        functools.partial(land_kernel, sz),
        in_specs=[SMEM, SMEM] + [VMEM] * (2 * c) + [ANY] * 3,
        out_specs=[ANY] * 3,
        out_shape=[jax.ShapeDtypeStruct(o.shape, o.dtype) for o in outs],
        scratch_shapes=[
            pltpu.VMEM((3, c, sz.piece, sz.cols), f32),
            pltpu.VMEM((3, sz.layers, sz.rows, sz.cols), f32),
            pltpu.SemaphoreType.DMA((3, sz.layers)),
        ],
        input_output_aliases={2 + 2 * c + a: a for a in range(3)},
        name="land",
    )(me, plan, *early, *late, *outs)


def spread(sz, arrays):
    c = sz.chips
    got = [arrays[0]]
    for x in range(1, c):
        pairs = [
            (i * CORES + k, peer(i, x, c) * CORES + k) for i in range(c) for k in range(CORES)
        ]
        got.append(lax.ppermute(arrays[x], "expert", pairs))
    return got[:1] + near(got[1:])


def from_others(value, axis):
    n = lax.axis_size(axis)
    return sum(
        lax.ppermute(value, axis, [(i, peer(i, x, n)) for i in range(n)]) for x in range(1, n)
    )


def swap(sz, arrays):
    pairs = [(i, i ^ 1) for i in range(sz.group)]
    return [lax.ppermute(a, "expert", pairs) for a in arrays]


def shards(master, moment_one, moment_two, gradient, old_slot, new_slot):
    sz = Sizes(master.shape, lax.axis_size("expert"), lax.axis_size("dp"))
    me = lax.axis_index("expert").reshape(1)
    c = sz.chips
    got = prep(sz, me, old_slot, new_slot, master, moment_one, moment_two, gradient)
    pieces, late, plan = list(got[:c]), list(got[c : 2 * c]), got[2 * c]
    held = spread(sz, pieces)
    total = squares(sz, gradient)
    total = total + swap(sz, [total])[0]
    total = total + from_others(total, "dp")
    totals = spread(sz, [total] * c)
    late_held = spread(sz, late)
    clip = clip_scale(sz, totals)
    other = near(swap(sz, held))
    early_out = pick(sz, 0, me, plan, clip, held, other)
    early_in = spread(sz, list(early_out))
    late_other = near(swap(sz, late_held))
    late_out = pick(sz, 1, me, plan, clip, late_held, late_other)
    late_in = spread(sz, list(late_out))
    scale = clip[0, 0]
    wide = gradient.astype(jnp.float32)
    first, second = moments(moment_one, moment_two, wide, scale)
    weights = new_weights(master, first, second)
    return tuple(land(sz, me, plan, early_in, late_in, (weights, first, second)))


def solution(mesh):
    spec = P(None, "expert", "dp", None)
    return jax.shard_map(
        shards,
        mesh=mesh,
        in_specs=(spec, spec, spec, spec, P(), P()),
        out_specs=(spec, spec, spec),
        check_vma=False,
    )
```

```python
import functools
import math

import jax
import jax.numpy as jnp
from jax import lax
from jax.experimental import pallas as pl
from jax.experimental.pallas import tpu as pltpu
from jax.sharding import PartitionSpec as P


BETA_ONE = 0.9
BETA_TWO = 0.95
LEARN_RATE = 0.05
DECAY_RATE = 0.1
ADAM_EPS = 1e-08
CLIP_RMS = 2.0
FIRST_FIX = 1.0 - 0.9**10
SECOND_FIX = 1.0 - 0.95**10

LANES = 128
CORES = 2
EARLY = 0.25

ANY = pl.BlockSpec(memory_space=pl.ANY)
SMEM = pl.BlockSpec(memory_space=pltpu.SMEM)
VMEM = pl.BlockSpec(memory_space=pltpu.VMEM)


def out(*shape, dtype=jnp.float32):
    return pltpu.VMEM(shape, dtype)


def near(arrays):
    return [pltpu.with_memory_space_constraint(a, pltpu.VMEM) for a in arrays]


def up(n):
    return -(-n // LANES) * LANES


def moments(moment_one, moment_two, gradient, clip_scale):
    scaled = gradient * clip_scale
    first = BETA_ONE * moment_one + (1.0 - BETA_ONE) * scaled
    second = BETA_TWO * moment_two + (1.0 - BETA_TWO) * scaled * scaled
    return first, second


def new_weights(master, first, second):
    step_dir = first / FIRST_FIX / (jnp.sqrt(second / SECOND_FIX) + ADAM_EPS)
    return master - LEARN_RATE * (step_dir + DECAY_RATE * master)


class Sizes:
    def __init__(self, shape, group, dp):
        self.layers, self.slots, self.rows, self.cols = shape
        self.group = group
        self.devices = group * dp
        self.chips = group // CORES
        self.piece = self.layers * self.rows // self.chips
        self.per_layer = self.rows // self.piece
        early = round(self.cols * EARLY / LANES) * LANES
        self.early = early
        self.late = self.cols - early
        self.lat = up(self.late)
        self.full = up(self.cols)
        self.groups = ((self.full, 0, early, early), (0, early, self.late, self.lat))


def width(group, parts):
    head, _, _, stride = group
    return head + parts * stride


def peer(i, x, n):
    return i ^ x if n & (n - 1) == 0 else (i + x) % n


def dyn_peer(i, x, n):
    return i ^ x if n & (n - 1) == 0 else lax.rem(i + x, n)


def prep_kernel(sz, me_ref, old_ref, new_ref, master, mone, mtwo, grad, *rest):
    c = sz.chips
    pieces = rest[:c]
    late_raw, total, plan, mv, m1v, m2v, gv, st, sem_g, sem = rest[c:]
    for i in range(sz.layers):
        pltpu.make_async_copy(grad.at[i], gv.at[i], sem_g.at[i]).start()
    me = me_ref[0]
    chip = lax.div(me, CORES)
    n_slots = sz.layers * sz.group

    for i in range(sz.layers):
        def note(e, carry):
            o = old_ref[i, e]
            n = new_ref[i, e]
            place = jnp.where(o != n, i * sz.group + lax.div(n, sz.slots), n_slots)
            plan[0, place] = lax.div(o, sz.slots)
            plan[1, place] = lax.rem(n, sz.slots)
            return carry

        lax.fori_loop(0, old_ref.shape[1], note, 0, unroll=8)
        slot = plan[1, i * sz.group + me]
        for a, (src, dst) in enumerate(((master, mv), (mone, m1v), (mtwo, m2v))):
            pltpu.make_async_copy(src.at[i, slot], dst.at[i], sem.at[i, a]).start()
    acc = jnp.zeros((sz.rows, sz.cols), jnp.float32)
    for i in range(sz.layers):
        pltpu.make_async_copy(grad.at[i], gv.at[i], sem_g.at[i]).wait()
        for s in range(sz.slots):
            x = gv[i, s].astype(jnp.float32)
            acc = acc + x * x
    total[...] = jnp.broadcast_to(jnp.sum(acc), total.shape)
    for i in range(sz.layers):
        for a, (src, dst) in enumerate(((master, mv), (mone, m1v), (mtwo, m2v))):
            pltpu.make_async_copy(src.at[i, 0], dst.at[i], sem.at[i, a]).wait()
        g = gv[i, plan[1, i * sz.group + me]].astype(jnp.float32)
        for q in range(sz.per_layer):
            k = i * sz.per_layer + q
            r = slice(q * sz.piece, (q + 1) * sz.piece)
            st[0, k] = mv[i, r, :]
            st[1, k] = m1v[i, r, :]
            st[2, k] = m2v[i, r, :]
            st[3, k] = g[r, :]
    for x in range(c):
        k = dyn_peer(chip, x, c)
        pieces[x][:, : sz.cols] = st[0, k]
        for a in range(3):
            lo = sz.full + a * sz.early
            pieces[x][:, lo : lo + sz.early] = st[a + 1, k, :, : sz.early]
            late_raw[a, x] = st[a + 1, k, :, sz.early :]


def prep(sz, me, old_slot, new_slot, master, mone, mtwo, grad):
    f32 = jnp.float32
    slot = (sz.layers, sz.rows, sz.cols)
    outs = [out(sz.piece, width(sz.groups[0], 3))] * sz.chips + [
        out(3, sz.chips, sz.piece, sz.late),
        out(1, LANES),
        jax.ShapeDtypeStruct((2, sz.layers * sz.group + 1), jnp.int32),
    ]
    return pl.pallas_call(
        functools.partial(prep_kernel, sz),
        in_specs=[SMEM, SMEM, SMEM, ANY, ANY, ANY, ANY],
        out_specs=[VMEM] * (sz.chips + 2) + [SMEM],
        out_shape=outs,
        scratch_shapes=[
            pltpu.VMEM(slot, f32),
            pltpu.VMEM(slot, f32),
            pltpu.VMEM(slot, f32),
            pltpu.VMEM(grad.shape, grad.dtype),
            pltpu.VMEM((4, sz.chips, sz.piece, sz.cols), f32),
            pltpu.SemaphoreType.DMA((sz.layers,)),
            pltpu.SemaphoreType.DMA((sz.layers, 3)),
        ],
        name="prep",
    )(me, old_slot, new_slot, master, mone, mtwo, grad)


def scale_kernel(sz, total, raw, clip, *late):
    entries = sz.layers * sz.slots * sz.rows * sz.cols * sz.devices
    scale = jnp.minimum(
        1.0, CLIP_RMS * math.sqrt(entries) / (jnp.sqrt(total[...]) + 1e-06)
    )
    clip[...] = scale
    for x in range(sz.chips):
        first, second = moments(raw[0, x], raw[1, x], raw[2, x], scale[:, 0:1])
        late[x][:, : sz.late] = first
        late[x][:, sz.lat : sz.lat + sz.late] = second


def scale_and_late(sz, total, raw):
    return pl.pallas_call(
        functools.partial(scale_kernel, sz),
        in_specs=[VMEM, VMEM],
        out_specs=[VMEM] * (sz.chips + 1),
        out_shape=[out(1, LANES)] + [out(sz.piece, width(sz.groups[1], 2))] * sz.chips,
        name="scale_late",
    )(*near((total, raw)))


def pick_kernel(sz, group, me_ref, plan, clip, *rest):
    c = sz.chips
    refs = rest[: 2 * c]
    outs = rest[2 * c : 3 * c]
    head, _, size, stride = group
    at = [head + a * stride for a in range(3)]
    me = me_ref[0]
    chip = lax.div(me, CORES)
    core = lax.rem(me, CORES)
    layer = lax.div(chip, sz.per_layer)
    for x in range(c):
        target = dyn_peer(chip, x, c) * CORES + core
        sender = plan[0, layer * sz.group + target]
        from_chip = lax.div(sender, CORES)
        shift = from_chip ^ chip if c & (c - 1) == 0 else lax.rem(chip - from_chip + c, c)
        choice = shift + jnp.where(lax.rem(sender, CORES) == core, 0, c)
        for q in range(2 * c):
            @pl.when(choice == q)
            def _():
                if not head:
                    outs[x][...] = refs[q][...]
                    return
                parts = [refs[q][:, lo : lo + size] for lo in at]
                first, second = moments(*parts, clip[:, 0:1])
                outs[x][:, :head] = refs[q][:, :head]
                outs[x][:, at[0] : at[0] + size] = first
                outs[x][:, at[1] : at[1] + size] = second


def pick(sz, which, me, plan, clip, own, other):
    c = sz.chips
    group = sz.groups[which]
    return pl.pallas_call(
        functools.partial(pick_kernel, sz, group),
        in_specs=[SMEM, SMEM] + [VMEM] * (2 * c + 1),
        out_specs=[VMEM] * c,
        out_shape=[out(sz.piece, width(group, 2))] * c,
        name="pick",
    )(me, plan, clip, *own, *other)


def land_kernel(sz, me_ref, plan, *rest):
    c = sz.chips
    early, late = rest[:c], rest[c : 2 * c]
    outs = rest[2 * c + 3 : 2 * c + 6]
    st, full, sem = rest[2 * c + 6 :]
    me = me_ref[0]
    chip = lax.div(me, CORES)
    e, f = sz.early, sz.full
    for x in range(c):
        k = dyn_peer(chip, x, c) if c & (c - 1) == 0 else lax.rem(chip - x + c, c)
        a, b = early[x], late[x]
        first, second = a[:, f : f + e], a[:, f + e : f + 2 * e]
        st[0, k, :, :e] = new_weights(a[:, :e], first, second)
        st[1, k, :, :e] = first
        st[2, k, :, :e] = second
        first, second = b[:, : sz.late], b[:, sz.lat : sz.lat + sz.late]
        st[0, k, :, e:] = new_weights(a[:, e : sz.cols], first, second)
        st[1, k, :, e:] = first
        st[2, k, :, e:] = second
    copies = []
    for i in range(sz.layers):
        slot = plan[1, i * sz.group + me]
        for a in range(3):
            for q in range(sz.per_layer):
                r = slice(q * sz.piece, (q + 1) * sz.piece)
                full[a, i, r, :] = st[a, i * sz.per_layer + q]
            cp = pltpu.make_async_copy(full.at[a, i], outs[a].at[i, slot], sem.at[a, i])
            cp.start()
            copies.append(cp)
    for cp in copies:
        cp.wait()


def land(sz, me, plan, early, late, outs):
    f32 = jnp.float32
    c = sz.chips
    return pl.pallas_call(
        functools.partial(land_kernel, sz),
        in_specs=[SMEM, SMEM] + [VMEM] * (2 * c) + [ANY] * 3,
        out_specs=[ANY] * 3,
        out_shape=[jax.ShapeDtypeStruct(o.shape, o.dtype) for o in outs],
        scratch_shapes=[
            pltpu.VMEM((3, c, sz.piece, sz.cols), f32),
            pltpu.VMEM((3, sz.layers, sz.rows, sz.cols), f32),
            pltpu.SemaphoreType.DMA((3, sz.layers)),
        ],
        input_output_aliases={2 + 2 * c + a: a for a in range(3)},
        name="land",
    )(me, plan, *early, *late, *outs)


def shifts(sz, arrays):
    c = sz.chips
    got = [arrays[0]]
    for x in range(1, c):
        pairs = [
            (i * CORES + k, peer(i, x, c) * CORES + k) for i in range(c) for k in range(CORES)
        ]
        got.append(lax.ppermute(arrays[x], "expert", pairs))
    return got


def spread(sz, arrays):
    got = shifts(sz, arrays)
    return got[:1] + near(got[1:])


def from_others(value, axis):
    n = lax.axis_size(axis)
    return sum(
        lax.ppermute(value, axis, [(i, peer(i, x, n)) for i in range(n)]) for x in range(1, n)
    )


def swap(sz, arrays):
    pairs = [(i, i ^ 1) for i in range(sz.group)]
    return [lax.ppermute(a, "expert", pairs) for a in arrays]


def shards(master, moment_one, moment_two, gradient, old_slot, new_slot):
    sz = Sizes(master.shape, lax.axis_size("expert"), lax.axis_size("dp"))
    me = lax.axis_index("expert").reshape(1)
    c = sz.chips
    got = prep(sz, me, old_slot, new_slot, master, moment_one, moment_two, gradient)
    pieces, raw, total, plan = list(got[:c]), got[c], got[c + 1], got[c + 2]
    totals = shifts(sz, [total] * c)
    held = spread(sz, pieces)
    total = sum(totals)
    total = total + swap(sz, [total])[0]
    total = total + from_others(total, "dp")
    clip, *late = scale_and_late(sz, total, raw)
    late_held = spread(sz, late)
    other = near(swap(sz, held))
    early_out = pick(sz, 0, me, plan, clip, held, other)
    early_in = spread(sz, list(early_out))
    late_other = near(swap(sz, late_held))
    late_out = pick(sz, 1, me, plan, clip, late_held, late_other)
    late_in = spread(sz, list(late_out))
    scale = clip[0, 0]
    wide = gradient.astype(jnp.float32)
    first, second = moments(moment_one, moment_two, wide, scale)
    weights = new_weights(master, first, second)
    return tuple(land(sz, me, plan, early_in, late_in, (weights, first, second)))


def solution(mesh):
    spec = P(None, "expert", "dp", None)
    return jax.shard_map(
        shards,
        mesh=mesh,
        in_specs=(spec, spec, spec, spec, P(), P()),
        out_specs=(spec, spec, spec),
        check_vma=False,
    )
```

```python
import functools
import math

import jax
import jax.numpy as jnp
from jax import lax
from jax.experimental import pallas as pl
from jax.experimental.pallas import tpu as pltpu
from jax.sharding import PartitionSpec as P


BETA_ONE = 0.9
BETA_TWO = 0.95
LEARN_RATE = 0.05
DECAY_RATE = 0.1
ADAM_EPS = 1e-08
CLIP_RMS = 2.0
FIRST_FIX = 1.0 - 0.9**10
SECOND_FIX = 1.0 - 0.95**10

LANES = 128
CORES = 2
EARLY = 0.25

ANY = pl.BlockSpec(memory_space=pl.ANY)
SMEM = pl.BlockSpec(memory_space=pltpu.SMEM)
VMEM = pl.BlockSpec(memory_space=pltpu.VMEM)


def out(*shape, dtype=jnp.float32):
    return pltpu.VMEM(shape, dtype)


def near(arrays):
    return [pltpu.with_memory_space_constraint(a, pltpu.VMEM) for a in arrays]


def up(n):
    return -(-n // LANES) * LANES


def moments(moment_one, moment_two, gradient, clip_scale):
    scaled = gradient * clip_scale
    first = BETA_ONE * moment_one + (1.0 - BETA_ONE) * scaled
    second = BETA_TWO * moment_two + (1.0 - BETA_TWO) * scaled * scaled
    return first, second


def new_weights(master, first, second):
    step_dir = first / FIRST_FIX / (jnp.sqrt(second / SECOND_FIX) + ADAM_EPS)
    return master - LEARN_RATE * (step_dir + DECAY_RATE * master)


class Sizes:
    def __init__(self, shape, group, dp):
        self.layers, self.slots, self.rows, self.cols = shape
        self.group = group
        self.devices = group * dp
        self.chips = group // CORES
        self.order = [*range(self.chips // 2, self.chips), *range(1, self.chips // 2)]
        self.piece = self.layers * self.rows // self.chips
        self.per_layer = self.rows // self.piece
        self.by_piece = self.piece % 8 == 0
        early = round(self.cols * EARLY / LANES) * LANES
        self.early = early
        self.late = self.cols - early
        self.lat = up(self.late)
        self.full = up(self.cols)
        self.groups = ((self.full, 0, early, early), (0, early, self.late, self.lat))


def width(group, parts):
    head, _, _, stride = group
    return head + parts * stride


def peer(i, x, n):
    return i ^ x if n & (n - 1) == 0 else (i + x) % n


def dyn_peer(i, x, n):
    return i ^ x if n & (n - 1) == 0 else lax.rem(i + x, n)


def prep_kernel(sz, me_ref, old_ref, new_ref, master, mone, mtwo, grad, *rest):
    c = sz.chips
    pieces = rest[:c]
    late_raw, total, plan, mv, m1v, m2v, gv, st, sem_g, sem = rest[c:]
    for i in range(sz.layers):
        pltpu.make_async_copy(grad.at[i], gv.at[i], sem_g.at[i]).start()
    me = me_ref[0]
    chip = lax.div(me, CORES)
    n_slots = sz.layers * sz.group

    for i in range(sz.layers):
        def note(e, carry):
            o = old_ref[i, e]
            n = new_ref[i, e]
            place = jnp.where(o != n, i * sz.group + lax.div(n, sz.slots), n_slots)
            plan[0, place] = lax.div(o, sz.slots)
            plan[1, place] = lax.rem(n, sz.slots)
            return carry

        lax.fori_loop(0, old_ref.shape[1], note, 0, unroll=8)
        slot = plan[1, i * sz.group + me]
        for a, (src, dst) in enumerate(((master, mv), (mone, m1v), (mtwo, m2v))):
            pltpu.make_async_copy(src.at[i, slot], dst.at[i], sem.at[i, a]).start()
    acc = jnp.zeros((sz.rows, sz.cols), jnp.float32)
    for i in range(sz.layers):
        pltpu.make_async_copy(grad.at[i], gv.at[i], sem_g.at[i]).wait()
        for s in range(sz.slots):
            x = gv[i, s].astype(jnp.float32)
            acc = acc + x * x
    total[...] = jnp.broadcast_to(jnp.sum(acc), total.shape)
    for i in range(sz.layers):
        for a, (src, dst) in enumerate(((master, mv), (mone, m1v), (mtwo, m2v))):
            pltpu.make_async_copy(src.at[i, 0], dst.at[i], sem.at[i, a]).wait()
        g = gv[i, plan[1, i * sz.group + me]].astype(jnp.float32)
        for q in range(sz.per_layer):
            k = i * sz.per_layer + q
            r = slice(q * sz.piece, (q + 1) * sz.piece)
            st[0, k] = mv[i, r, :]
            st[1, k] = m1v[i, r, :]
            st[2, k] = m2v[i, r, :]
            st[3, k] = g[r, :]
    for x in range(c):
        k = dyn_peer(chip, x, c)
        pieces[x][:, : sz.cols] = st[0, k]
        for a in range(3):
            lo = sz.full + a * sz.early
            pieces[x][:, lo : lo + sz.early] = st[a + 1, k, :, : sz.early]
            late_raw[a, x] = st[a + 1, k, :, sz.early :]


def prep(sz, me, old_slot, new_slot, master, mone, mtwo, grad):
    f32 = jnp.float32
    slot = (sz.layers, sz.rows, sz.cols)
    outs = [out(sz.piece, width(sz.groups[0], 3))] * sz.chips + [
        out(3, sz.chips, sz.piece, sz.late),
        out(1, LANES),
        jax.ShapeDtypeStruct((2, sz.layers * sz.group + 1), jnp.int32),
    ]
    return pl.pallas_call(
        functools.partial(prep_kernel, sz),
        in_specs=[SMEM, SMEM, SMEM, ANY, ANY, ANY, ANY],
        out_specs=[VMEM] * (sz.chips + 2) + [SMEM],
        out_shape=outs,
        scratch_shapes=[
            pltpu.VMEM(slot, f32),
            pltpu.VMEM(slot, f32),
            pltpu.VMEM(slot, f32),
            pltpu.VMEM(grad.shape, grad.dtype),
            pltpu.VMEM((4, sz.chips, sz.piece, sz.cols), f32),
            pltpu.SemaphoreType.DMA((sz.layers,)),
            pltpu.SemaphoreType.DMA((sz.layers, 3)),
        ],
        name="prep",
    )(me, old_slot, new_slot, master, mone, mtwo, grad)


def scale_kernel(sz, total, raw, clip, clip_copy, *late):
    entries = sz.layers * sz.slots * sz.rows * sz.cols * sz.devices
    scale = jnp.minimum(
        1.0, CLIP_RMS * math.sqrt(entries) / (jnp.sqrt(total[...]) + 1e-06)
    )
    clip[...] = scale
    clip_copy[...] = scale
    for x in range(sz.chips):
        first, second = moments(raw[0, x], raw[1, x], raw[2, x], scale[:, 0:1])
        late[x][:, : sz.late] = first
        late[x][:, sz.lat : sz.lat + sz.late] = second


def scale_and_late(sz, total, raw):
    return pl.pallas_call(
        functools.partial(scale_kernel, sz),
        in_specs=[VMEM, VMEM],
        out_specs=[VMEM] * (sz.chips + 2),
        out_shape=[out(1, LANES), jax.ShapeDtypeStruct((1, LANES), jnp.float32)]
        + [out(sz.piece, width(sz.groups[1], 2))] * sz.chips,
        name="scale_late",
    )(*near((total, raw)))


def pick_kernel(sz, group, me_ref, plan, clip, *rest):
    c = sz.chips
    refs = rest[: 2 * c]
    outs = rest[2 * c : 3 * c]
    head, _, size, stride = group
    at = [head + a * stride for a in range(3)]
    me = me_ref[0]
    chip = lax.div(me, CORES)
    core = lax.rem(me, CORES)
    layer = lax.div(chip, sz.per_layer)
    for x in range(c):
        target = dyn_peer(chip, x, c) * CORES + core
        sender = plan[0, layer * sz.group + target]
        from_chip = lax.div(sender, CORES)
        shift = from_chip ^ chip if c & (c - 1) == 0 else lax.rem(chip - from_chip + c, c)
        choice = shift + jnp.where(lax.rem(sender, CORES) == core, 0, c)
        for q in range(2 * c):
            @pl.when(choice == q)
            def _():
                if not head:
                    outs[x][...] = refs[q][...]
                    return
                parts = [refs[q][:, lo : lo + size] for lo in at]
                first, second = moments(*parts, clip[:, 0:1])
                outs[x][:, :head] = refs[q][:, :head]
                outs[x][:, at[0] : at[0] + size] = first
                outs[x][:, at[1] : at[1] + size] = second


def pick(sz, which, me, plan, clip, own, other):
    c = sz.chips
    group = sz.groups[which]
    return pl.pallas_call(
        functools.partial(pick_kernel, sz, group),
        in_specs=[SMEM, SMEM] + [VMEM] * (2 * c + 1),
        out_specs=[VMEM] * c,
        out_shape=[out(sz.piece, width(group, 2))] * c,
        name="pick",
    )(me, plan, clip, *own, *other)


def land_kernel(sz, which, me_ref, plan, *rest):
    c, n = sz.chips, len(which)
    early, late = rest[:n], rest[n : 2 * n]
    outs = rest[2 * n + 3 : 2 * n + 6]
    st, full, sem = rest[2 * n + 6 :]
    me = me_ref[0]
    chip = lax.div(me, CORES)
    e, f = sz.early, sz.full
    copies = []
    for j, x in enumerate(which):
        k = dyn_peer(chip, x, c) if c & (c - 1) == 0 else lax.rem(chip - x + c, c)
        a, b = early[j], late[j]
        spot = j if sz.by_piece else k
        first, second = a[:, f : f + e], a[:, f + e : f + 2 * e]
        st[0, spot, :, :e] = new_weights(a[:, :e], first, second)
        st[1, spot, :, :e] = first
        st[2, spot, :, :e] = second
        first, second = b[:, : sz.late], b[:, sz.lat : sz.lat + sz.late]
        st[0, spot, :, e:] = new_weights(a[:, e : sz.cols], first, second)
        st[1, spot, :, e:] = first
        st[2, spot, :, e:] = second
        if sz.by_piece:
            layer = lax.div(k, sz.per_layer)
            row = pl.multiple_of(lax.rem(k, sz.per_layer) * sz.piece, sz.piece)
            slot = plan[1, layer * sz.group + me]
            for i in range(3):
                there = outs[i].at[layer, slot, pl.ds(row, sz.piece)]
                copies.append(pltpu.make_async_copy(st.at[i, j], there, sem.at[i, j]))
                copies[-1].start()
    if not sz.by_piece:
        for i in range(sz.layers):
            slot = plan[1, i * sz.group + me]
            for a in range(3):
                for q in range(sz.per_layer):
                    r = slice(q * sz.piece, (q + 1) * sz.piece)
                    full[a, i, r, :] = st[a, i * sz.per_layer + q]
                copies.append(
                    pltpu.make_async_copy(full.at[a, i], outs[a].at[i, slot], sem.at[a, i])
                )
                copies[-1].start()
    for cp in copies:
        cp.wait()


def land(sz, which, me, plan, early, late, outs):
    f32 = jnp.float32
    n = len(which)
    whole = (8, LANES) if sz.by_piece else (3, sz.layers, sz.rows, sz.cols)
    return pl.pallas_call(
        functools.partial(land_kernel, sz, which),
        in_specs=[SMEM, SMEM] + [VMEM] * (2 * n) + [ANY] * 3,
        out_specs=[ANY] * 3,
        out_shape=[jax.ShapeDtypeStruct(o.shape, o.dtype) for o in outs],
        scratch_shapes=[
            pltpu.VMEM((3, n, sz.piece, sz.cols), f32),
            pltpu.VMEM(whole, f32),
            pltpu.SemaphoreType.DMA((3, max(n, sz.layers))),
        ],
        input_output_aliases={2 + 2 * n + a: a for a in range(3)},
        name="land",
    )(me, plan, *[early[x] for x in which], *[late[x] for x in which], *outs)


def shifts(sz, arrays):
    c = sz.chips
    got = [arrays[0]] * c
    for x in sz.order:
        pairs = [
            (i * CORES + k, peer(i, x, c) * CORES + k) for i in range(c) for k in range(CORES)
        ]
        got[x] = lax.ppermute(arrays[x], "expert", pairs)
    return got


def spread(sz, arrays):
    return near(shifts(sz, arrays))


def from_others(value, axis):
    n = lax.axis_size(axis)
    return sum(
        lax.ppermute(value, axis, [(i, peer(i, x, n)) for i in range(n)]) for x in range(1, n)
    )


def swap(sz, arrays):
    pairs = [(i, i ^ 1) for i in range(sz.group)]
    return [lax.ppermute(a, "expert", pairs) for a in arrays]


def shards(master, moment_one, moment_two, gradient, old_slot, new_slot):
    sz = Sizes(master.shape, lax.axis_size("expert"), lax.axis_size("dp"))
    me = lax.axis_index("expert").reshape(1)
    c = sz.chips
    got = prep(sz, me, old_slot, new_slot, master, moment_one, moment_two, gradient)
    pieces, raw, total, plan = list(got[:c]), got[c], got[c + 1], got[c + 2]
    totals = shifts(sz, [total] * c)
    held = spread(sz, pieces)
    total = sum(totals)
    total = total + swap(sz, [total])[0]
    total = total + from_others(total, "dp")
    clip, clip_copy, *late = scale_and_late(sz, total, raw)
    (clip,) = near([clip])
    late_held = spread(sz, late)
    other = near(swap(sz, held))
    early_out = pick(sz, 0, me, plan, clip, held, other)
    early_in = spread(sz, list(early_out))
    late_other = near(swap(sz, late_held))
    late_out = pick(sz, 1, me, plan, clip, late_held, late_other)
    late_in = spread(sz, list(late_out))
    scale = clip_copy[0, 0]
    wide = gradient.astype(jnp.float32)
    first, second = moments(moment_one, moment_two, wide, scale)
    weights = new_weights(master, first, second)
    outs = (weights, first, second)
    half = c // 2
    batches = [range(half), range(half, c)] if sz.by_piece else [range(c)]
    for which in batches:
        outs = land(sz, list(which), me, plan, early_in, late_in, outs)
    return tuple(outs)


def solution(mesh):
    spec = P(None, "expert", "dp", None)
    return jax.shard_map(
        shards,
        mesh=mesh,
        in_specs=(spec, spec, spec, spec, P(), P()),
        out_specs=(spec, spec, spec),
        check_vma=False,
    )
```

```python
import functools
import math

import jax
import jax.numpy as jnp
from jax import lax
from jax.experimental import pallas as pl
from jax.experimental.pallas import tpu as pltpu
from jax.sharding import PartitionSpec as P


BETA_ONE = 0.9
BETA_TWO = 0.95
LEARN_RATE = 0.05
DECAY_RATE = 0.1
ADAM_EPS = 1e-08
CLIP_RMS = 2.0
FIRST_FIX = 1.0 - 0.9**10
SECOND_FIX = 1.0 - 0.95**10

LANES = 128
CORES = 2
EARLY = 0.18

ANY = pl.BlockSpec(memory_space=pl.ANY)
SMEM = pl.BlockSpec(memory_space=pltpu.SMEM)
VMEM = pl.BlockSpec(memory_space=pltpu.VMEM)


def out(*shape, dtype=jnp.float32):
    return pltpu.VMEM(shape, dtype)


def near(arrays):
    return [pltpu.with_memory_space_constraint(a, pltpu.VMEM) for a in arrays]


def up(n):
    return -(-n // LANES) * LANES


def moments(moment_one, moment_two, gradient, clip_scale):
    scaled = gradient * clip_scale
    first = BETA_ONE * moment_one + (1.0 - BETA_ONE) * scaled
    second = BETA_TWO * moment_two + (1.0 - BETA_TWO) * scaled * scaled
    return first, second


def new_weights(master, first, second):
    step_dir = first / FIRST_FIX / (jnp.sqrt(second / SECOND_FIX) + ADAM_EPS)
    return master - LEARN_RATE * (step_dir + DECAY_RATE * master)


class Sizes:
    def __init__(self, shape, group, dp):
        self.layers, self.slots, self.rows, self.cols = shape
        self.group = group
        self.devices = group * dp
        self.chips = group // CORES
        self.order = [*range(self.chips // 2, self.chips), *range(1, self.chips // 2)]
        self.piece = self.layers * self.rows // self.chips
        self.per_layer = self.rows // self.piece
        self.by_piece = self.piece % 8 == 0
        early = round(self.cols * EARLY / LANES) * LANES
        self.early = early
        self.late = self.cols - early
        self.lat = self.late if self.late % (LANES // 2) == 0 else up(self.late)
        self.full = up(self.cols)
        self.groups = ((self.full, 0, early, early), (0, early, self.late, self.lat))


def width(group, parts):
    head, _, _, stride = group
    return head + parts * stride


def read(note, place):
    lane = lax.broadcasted_iota(jnp.int32, note.shape, 1)
    return jnp.max(jnp.where(lane == place, note[...], 0))


def peer(i, x, n):
    return i ^ x if n & (n - 1) == 0 else (i + x) % n


def dyn_peer(i, x, n):
    return i ^ x if n & (n - 1) == 0 else lax.rem(i + x, n)


def prep_kernel(sz, me_ref, old_ref, new_ref, master, mone, mtwo, grad, *rest):
    c = sz.chips
    pieces = rest[:c]
    late_raw, notes, plan, mv, m1v, m2v, gv, st, sem = rest[c:]
    me = me_ref[0]
    chip = lax.div(me, CORES)
    n_slots = sz.layers * sz.group

    for i in range(sz.layers):
        def note(e, carry):
            o = old_ref[i, e]
            n = new_ref[i, e]
            place = jnp.where(o != n, i * sz.group + lax.div(n, sz.slots), n_slots)
            plan[0, place] = lax.div(o, sz.slots)
            plan[1, place] = lax.rem(n, sz.slots)
            return carry

        lax.fori_loop(0, old_ref.shape[1], note, 0, unroll=8)
        slot = plan[1, i * sz.group + me]
        for a, (src, dst) in enumerate(((master, mv), (mone, m1v), (mtwo, m2v), (grad, gv))):
            pltpu.make_async_copy(src.at[i, slot], dst.at[i], sem.at[i, a]).start()
    for i in range(sz.layers):
        for a, (src, dst) in enumerate(((master, mv), (mone, m1v), (mtwo, m2v), (grad, gv))):
            pltpu.make_async_copy(src.at[i, 0], dst.at[i], sem.at[i, a]).wait()
        g = gv[i].astype(jnp.float32)
        for q in range(sz.per_layer):
            k = i * sz.per_layer + q
            r = slice(q * sz.piece, (q + 1) * sz.piece)
            st[0, k] = mv[i, r, :]
            st[1, k] = m1v[i, r, :]
            st[2, k] = m2v[i, r, :]
            st[3, k] = g[r, :]
    lane = lax.broadcasted_iota(jnp.int32, notes.shape, 1)
    table = jnp.where(lane == n_slots + sz.layers, me, 0)
    for i in range(n_slots):
        table = jnp.where(lane == i, plan[0, i], table)
    for i in range(sz.layers):
        table = jnp.where(lane == n_slots + i, plan[1, i * sz.group + me], table)
    notes[...] = table
    for x in range(c):
        k = dyn_peer(chip, x, c)
        pieces[x][:, : sz.cols] = st[0, k]
        for a in range(3):
            lo = sz.full + a * sz.early
            pieces[x][:, lo : lo + sz.early] = st[a + 1, k, :, : sz.early]
            late_raw[a, x] = st[a + 1, k, :, sz.early :]


def prep(sz, me, old_slot, new_slot, master, mone, mtwo, grad):
    f32 = jnp.float32
    slot = (sz.layers, sz.rows, sz.cols)
    outs = [out(sz.piece, width(sz.groups[0], 3))] * sz.chips + [
        out(3, sz.chips, sz.piece, sz.late),
        out(1, up(sz.layers * (sz.group + 1) + 1), dtype=jnp.int32),
    ]
    return pl.pallas_call(
        functools.partial(prep_kernel, sz),
        in_specs=[SMEM, SMEM, SMEM, ANY, ANY, ANY, ANY],
        out_specs=[VMEM] * (sz.chips + 2),
        out_shape=outs,
        scratch_shapes=[
            pltpu.SMEM((2, sz.layers * sz.group + 1), jnp.int32),
            pltpu.VMEM(slot, f32),
            pltpu.VMEM(slot, f32),
            pltpu.VMEM(slot, f32),
            pltpu.VMEM(slot, grad.dtype),
            pltpu.VMEM((4, sz.chips, sz.piece, sz.cols), f32),
            pltpu.SemaphoreType.DMA((sz.layers, 4)),
        ],
        name="prep",
    )(me, old_slot, new_slot, master, mone, mtwo, grad)


def square_kernel(sz, grad, total, gv, sem):
    copies = [pltpu.make_async_copy(grad.at[i], gv.at[i], sem.at[i]) for i in range(sz.layers)]
    for cp in copies:
        cp.start()
    acc = jnp.zeros((sz.rows, sz.cols), jnp.float32)
    for i in range(sz.layers):
        copies[i].wait()
        for s in range(sz.slots):
            x = gv[i, s].astype(jnp.float32)
            acc = acc + x * x
    total[...] = jnp.broadcast_to(jnp.sum(acc), total.shape)


def squares(sz, grad):
    return pl.pallas_call(
        functools.partial(square_kernel, sz),
        in_specs=[ANY],
        out_specs=VMEM,
        out_shape=out(1, LANES),
        scratch_shapes=[
            pltpu.VMEM(grad.shape, grad.dtype),
            pltpu.SemaphoreType.DMA((sz.layers,)),
        ],
        name="squares",
    )(grad)


def scale_kernel(sz, total, raw, clip, clip_copy, *late):
    entries = sz.layers * sz.slots * sz.rows * sz.cols * sz.devices
    scale = jnp.minimum(
        1.0, CLIP_RMS * math.sqrt(entries) / (jnp.sqrt(total[...]) + 1e-06)
    )
    clip[...] = scale
    clip_copy[...] = scale
    for x in range(sz.chips):
        first, second = moments(raw[0, x], raw[1, x], raw[2, x], scale[:, 0:1])
        late[x][:, : sz.late] = first
        late[x][:, sz.lat : sz.lat + sz.late] = second


def scale_and_late(sz, total, raw):
    return pl.pallas_call(
        functools.partial(scale_kernel, sz),
        in_specs=[VMEM, VMEM],
        out_specs=[VMEM] * (sz.chips + 2),
        out_shape=[out(1, LANES), jax.ShapeDtypeStruct((1, LANES), jnp.float32)]
        + [out(sz.piece, width(sz.groups[1], 2))] * sz.chips,
        name="scale_late",
    )(*near((total, raw)))


def pick_kernel(sz, group, notes, clip, *rest):
    c = sz.chips
    refs = rest[: 2 * c]
    outs = rest[2 * c : 3 * c]
    head, _, size, stride = group
    at = [head + a * stride for a in range(3)]
    me = read(notes, sz.layers * (sz.group + 1))
    chip = lax.div(me, CORES)
    core = lax.rem(me, CORES)
    layer = lax.div(chip, sz.per_layer)
    for x in range(c):
        target = dyn_peer(chip, x, c) * CORES + core
        sender = read(notes, layer * sz.group + target)
        from_chip = lax.div(sender, CORES)
        shift = from_chip ^ chip if c & (c - 1) == 0 else lax.rem(chip - from_chip + c, c)
        choice = shift + jnp.where(lax.rem(sender, CORES) == core, 0, c)
        for q in range(2 * c):
            @pl.when(choice == q)
            def _():
                if not head:
                    outs[x][...] = refs[q][...]
                    return
                parts = [refs[q][:, lo : lo + size] for lo in at]
                first, second = moments(*parts, clip[:, 0:1])
                outs[x][:, :head] = refs[q][:, :head]
                outs[x][:, at[0] : at[0] + size] = first
                outs[x][:, at[1] : at[1] + size] = second


def pick(sz, which, notes, clip, own, other):
    c = sz.chips
    group = sz.groups[which]
    return pl.pallas_call(
        functools.partial(pick_kernel, sz, group),
        in_specs=[VMEM] * (2 * c + 2),
        out_specs=[VMEM] * c,
        out_shape=[out(sz.piece, width(group, 2))] * c,
        name="pick",
    )(notes, clip, *own, *other)


def land_kernel(sz, which, notes, *rest):
    c, n = sz.chips, len(which)
    early, late = rest[:n], rest[n : 2 * n]
    outs = rest[2 * n + 3 : 2 * n + 6]
    st, full, sem = rest[2 * n + 6 :]
    n_slots = sz.layers * sz.group
    chip = lax.div(read(notes, n_slots + sz.layers), CORES)
    e, f = sz.early, sz.full
    copies = []
    for j, x in enumerate(which):
        k = dyn_peer(chip, x, c) if c & (c - 1) == 0 else lax.rem(chip - x + c, c)
        a, b = early[j], late[j]
        spot = j if sz.by_piece else k
        first, second = a[:, f : f + e], a[:, f + e : f + 2 * e]
        st[0, spot, :, :e] = new_weights(a[:, :e], first, second)
        st[1, spot, :, :e] = first
        st[2, spot, :, :e] = second
        first, second = b[:, : sz.late], b[:, sz.lat : sz.lat + sz.late]
        st[0, spot, :, e:] = new_weights(a[:, e : sz.cols], first, second)
        st[1, spot, :, e:] = first
        st[2, spot, :, e:] = second
        if sz.by_piece:
            layer = lax.div(k, sz.per_layer)
            row = pl.multiple_of(lax.rem(k, sz.per_layer) * sz.piece, sz.piece)
            slot = read(notes, n_slots + layer)
            for i in range(3):
                there = outs[i].at[layer, slot, pl.ds(row, sz.piece)]
                copies.append(pltpu.make_async_copy(st.at[i, j], there, sem.at[i, j]))
                copies[-1].start()
    if not sz.by_piece:
        for i in range(sz.layers):
            slot = read(notes, n_slots + i)
            for a in range(3):
                for q in range(sz.per_layer):
                    r = slice(q * sz.piece, (q + 1) * sz.piece)
                    full[a, i, r, :] = st[a, i * sz.per_layer + q]
                copies.append(
                    pltpu.make_async_copy(full.at[a, i], outs[a].at[i, slot], sem.at[a, i])
                )
                copies[-1].start()
    for cp in copies:
        cp.wait()


def land(sz, which, notes, early, late, outs):
    f32 = jnp.float32
    n = len(which)
    whole = (8, LANES) if sz.by_piece else (3, sz.layers, sz.rows, sz.cols)
    return pl.pallas_call(
        functools.partial(land_kernel, sz, which),
        in_specs=[VMEM] * (2 * n + 1) + [ANY] * 3,
        out_specs=[ANY] * 3,
        out_shape=[jax.ShapeDtypeStruct(o.shape, o.dtype) for o in outs],
        scratch_shapes=[
            pltpu.VMEM((3, n, sz.piece, sz.cols), f32),
            pltpu.VMEM(whole, f32),
            pltpu.SemaphoreType.DMA((3, max(n, sz.layers))),
        ],
        input_output_aliases={1 + 2 * n + a: a for a in range(3)},
        name="land",
    )(notes, *[early[x] for x in which], *[late[x] for x in which], *outs)


def shifts(sz, arrays):
    c = sz.chips
    got = [arrays[0]] * c
    for x in sz.order:
        pairs = [
            (i * CORES + k, peer(i, x, c) * CORES + k) for i in range(c) for k in range(CORES)
        ]
        got[x] = lax.ppermute(arrays[x], "expert", pairs)
    return got


def spread(sz, arrays):
    return near(shifts(sz, arrays))


def from_others(value, axis):
    n = lax.axis_size(axis)
    return sum(
        lax.ppermute(value, axis, [(i, peer(i, x, n)) for i in range(n)]) for x in range(1, n)
    )


def swap(sz, arrays):
    pairs = [(i, i ^ 1) for i in range(sz.group)]
    return [lax.ppermute(a, "expert", pairs) for a in arrays]


def shards(master, moment_one, moment_two, gradient, old_slot, new_slot):
    sz = Sizes(master.shape, lax.axis_size("expert"), lax.axis_size("dp"))
    me = lax.axis_index("expert").reshape(1)
    c = sz.chips
    total = squares(sz, gradient)
    totals = shifts(sz, [total] * c)
    got = prep(sz, me, old_slot, new_slot, master, moment_one, moment_two, gradient)
    pieces, raw = list(got[:c]), got[c]
    (notes,) = near([got[c + 1]])
    held = spread(sz, pieces)
    total = sum(totals)
    total = total + swap(sz, [total])[0]
    total = total + from_others(total, "dp")
    clip, clip_copy, *late = scale_and_late(sz, total, raw)
    (clip,) = near([clip])
    late_held = spread(sz, late)
    other = near(swap(sz, held))
    early_out = pick(sz, 0, notes, clip, held, other)
    early_in = spread(sz, list(early_out))
    late_other = near(swap(sz, late_held))
    late_out = pick(sz, 1, notes, clip, late_held, late_other)
    late_in = spread(sz, list(late_out))
    scale = clip_copy[0, 0]
    wide = gradient.astype(jnp.float32)
    first, second = moments(moment_one, moment_two, wide, scale)
    weights = new_weights(master, first, second)
    outs = (weights, first, second)
    half = c // 2
    batches = [range(half), range(half, c)] if sz.by_piece else [range(c)]
    for which in batches:
        outs = land(sz, list(which), notes, early_in, late_in, outs)
    return tuple(outs)


def solution(mesh):
    spec = P(None, "expert", "dp", None)
    return jax.shard_map(
        shards,
        mesh=mesh,
        in_specs=(spec, spec, spec, spec, P(), P()),
        out_specs=(spec, spec, spec),
        check_vma=False,
    )
```

```python
import functools
import math

import jax
import jax.numpy as jnp
from jax import lax
from jax.experimental import pallas as pl
from jax.experimental.pallas import tpu as pltpu
from jax.sharding import PartitionSpec as P


BETA_ONE = 0.9
BETA_TWO = 0.95
LEARN_RATE = 0.05
DECAY_RATE = 0.1
ADAM_EPS = 1e-08
CLIP_RMS = 2.0
FIRST_FIX = 1.0 - 0.9**10
SECOND_FIX = 1.0 - 0.95**10

LANES = 128
CORES = 2
EARLY = 0.18

ANY = pl.BlockSpec(memory_space=pl.ANY)
SMEM = pl.BlockSpec(memory_space=pltpu.SMEM)
VMEM = pl.BlockSpec(memory_space=pltpu.VMEM)


def out(*shape, dtype=jnp.float32):
    return pltpu.VMEM(shape, dtype)


def near(arrays):
    return [pltpu.with_memory_space_constraint(a, pltpu.VMEM) for a in arrays]


def up(n):
    return -(-n // LANES) * LANES


def moments(moment_one, moment_two, gradient, clip_scale):
    scaled = gradient * clip_scale
    first = BETA_ONE * moment_one + (1.0 - BETA_ONE) * scaled
    second = BETA_TWO * moment_two + (1.0 - BETA_TWO) * scaled * scaled
    return first, second


def new_weights(master, first, second):
    step_dir = first / FIRST_FIX / (jnp.sqrt(second / SECOND_FIX) + ADAM_EPS)
    return master - LEARN_RATE * (step_dir + DECAY_RATE * master)


class Sizes:
    def __init__(self, shape, group, dp):
        self.layers, self.slots, self.rows, self.cols = shape
        self.group = group
        self.devices = group * dp
        self.chips = group // CORES
        self.order = [*range(self.chips // 2, self.chips), *range(1, self.chips // 2)]
        self.piece = self.layers * self.rows // self.chips
        self.per_layer = self.rows // self.piece
        self.by_piece = self.piece % 8 == 0
        early = round(self.cols * EARLY / LANES) * LANES
        self.early = early
        self.late = self.cols - early
        self.lat = self.late if self.late % (LANES // 2) == 0 else up(self.late)
        self.full = up(self.cols)
        self.groups = ((self.full, 0, early, early), (0, early, self.late, self.lat))


def width(group, parts):
    head, _, _, stride = group
    return head + parts * stride


def read(note, place):
    lane = lax.broadcasted_iota(jnp.int32, note.shape, 1)
    return jnp.max(jnp.where(lane == place, note[...], 0))


def peer(i, x, n):
    return i ^ x if n & (n - 1) == 0 else (i + x) % n


def dyn_peer(i, x, n):
    return i ^ x if n & (n - 1) == 0 else lax.rem(i + x, n)


def prep_kernel(sz, me_ref, old_ref, new_ref, master, mone, mtwo, grad, *rest):
    c = sz.chips
    pieces = rest[:c]
    late_raw, total, notes, plan, mv, m1v, m2v, gv, st, sem_g, sem = rest[c:]
    for i in range(sz.layers):
        pltpu.make_async_copy(grad.at[i], gv.at[i], sem_g.at[i]).start()
    me = me_ref[0]
    chip = lax.div(me, CORES)
    n_slots = sz.layers * sz.group

    for i in range(sz.layers):
        def note(e, carry):
            o = old_ref[i, e]
            n = new_ref[i, e]
            place = jnp.where(o != n, i * sz.group + lax.div(n, sz.slots), n_slots)
            plan[0, place] = lax.div(o, sz.slots)
            plan[1, place] = lax.rem(n, sz.slots)
            return carry

        lax.fori_loop(0, old_ref.shape[1], note, 0, unroll=8)
        slot = plan[1, i * sz.group + me]
        for a, (src, dst) in enumerate(((master, mv), (mone, m1v), (mtwo, m2v))):
            pltpu.make_async_copy(src.at[i, slot], dst.at[i], sem.at[i, a]).start()
    acc = jnp.zeros((sz.rows, sz.cols), jnp.float32)
    for i in range(sz.layers):
        pltpu.make_async_copy(grad.at[i], gv.at[i], sem_g.at[i]).wait()
        for s in range(sz.slots):
            x = gv[i, s].astype(jnp.float32)
            acc = acc + x * x
    total[...] = jnp.broadcast_to(jnp.sum(acc), total.shape)
    for i in range(sz.layers):
        for a, (src, dst) in enumerate(((master, mv), (mone, m1v), (mtwo, m2v))):
            pltpu.make_async_copy(src.at[i, 0], dst.at[i], sem.at[i, a]).wait()
        g = gv[i, plan[1, i * sz.group + me]].astype(jnp.float32)
        for q in range(sz.per_layer):
            k = i * sz.per_layer + q
            r = slice(q * sz.piece, (q + 1) * sz.piece)
            st[0, k] = mv[i, r, :]
            st[1, k] = m1v[i, r, :]
            st[2, k] = m2v[i, r, :]
            st[3, k] = g[r, :]
    lane = lax.broadcasted_iota(jnp.int32, notes.shape, 1)
    table = jnp.where(lane == n_slots + sz.layers, me, 0)
    for i in range(n_slots):
        table = jnp.where(lane == i, plan[0, i], table)
    for i in range(sz.layers):
        table = jnp.where(lane == n_slots + i, plan[1, i * sz.group + me], table)
    notes[...] = table
    for x in range(c):
        k = dyn_peer(chip, x, c)
        pieces[x][:, : sz.cols] = st[0, k]
        for a in range(3):
            lo = sz.full + a * sz.early
            pieces[x][:, lo : lo + sz.early] = st[a + 1, k, :, : sz.early]
            late_raw[a, x] = st[a + 1, k, :, sz.early :]


def prep(sz, me, old_slot, new_slot, master, mone, mtwo, grad):
    f32 = jnp.float32
    slot = (sz.layers, sz.rows, sz.cols)
    outs = [out(sz.piece, width(sz.groups[0], 3))] * sz.chips + [
        out(3, sz.chips, sz.piece, sz.late),
        out(1, LANES),
        out(1, up(sz.layers * (sz.group + 1) + 1), dtype=jnp.int32),
    ]
    return pl.pallas_call(
        functools.partial(prep_kernel, sz),
        in_specs=[SMEM, SMEM, SMEM, ANY, ANY, ANY, ANY],
        out_specs=[VMEM] * (sz.chips + 3),
        out_shape=outs,
        scratch_shapes=[
            pltpu.SMEM((2, sz.layers * sz.group + 1), jnp.int32),
            pltpu.VMEM(slot, f32),
            pltpu.VMEM(slot, f32),
            pltpu.VMEM(slot, f32),
            pltpu.VMEM(grad.shape, grad.dtype),
            pltpu.VMEM((4, sz.chips, sz.piece, sz.cols), f32),
            pltpu.SemaphoreType.DMA((sz.layers,)),
            pltpu.SemaphoreType.DMA((sz.layers, 3)),
        ],
        name="prep",
    )(me, old_slot, new_slot, master, mone, mtwo, grad)


def scale_kernel(sz, total, raw, clip, clip_copy, *late):
    entries = sz.layers * sz.slots * sz.rows * sz.cols * sz.devices
    scale = jnp.minimum(
        1.0, CLIP_RMS * math.sqrt(entries) / (jnp.sqrt(total[...]) + 1e-06)
    )
    clip[...] = scale
    clip_copy[...] = scale
    for x in range(sz.chips):
        first, second = moments(raw[0, x], raw[1, x], raw[2, x], scale[:, 0:1])
        late[x][:, : sz.late] = first
        late[x][:, sz.lat : sz.lat + sz.late] = second


def scale_and_late(sz, total, raw):
    return pl.pallas_call(
        functools.partial(scale_kernel, sz),
        in_specs=[VMEM, VMEM],
        out_specs=[VMEM] * (sz.chips + 2),
        out_shape=[out(1, LANES), jax.ShapeDtypeStruct((1, LANES), jnp.float32)]
        + [out(sz.piece, width(sz.groups[1], 2))] * sz.chips,
        name="scale_late",
    )(*near((total, raw)))


def pick_kernel(sz, group, notes, clip, *rest):
    c = sz.chips
    refs = rest[: 2 * c]
    outs = rest[2 * c : 3 * c]
    head, _, size, stride = group
    at = [head + a * stride for a in range(3)]
    me = read(notes, sz.layers * (sz.group + 1))
    chip = lax.div(me, CORES)
    core = lax.rem(me, CORES)
    layer = lax.div(chip, sz.per_layer)
    for x in range(c):
        target = dyn_peer(chip, x, c) * CORES + core
        sender = read(notes, layer * sz.group + target)
        from_chip = lax.div(sender, CORES)
        shift = from_chip ^ chip if c & (c - 1) == 0 else lax.rem(chip - from_chip + c, c)
        choice = shift + jnp.where(lax.rem(sender, CORES) == core, 0, c)
        for q in range(2 * c):
            @pl.when(choice == q)
            def _():
                if not head:
                    outs[x][...] = refs[q][...]
                    return
                parts = [refs[q][:, lo : lo + size] for lo in at]
                first, second = moments(*parts, clip[:, 0:1])
                outs[x][:, :head] = refs[q][:, :head]
                outs[x][:, at[0] : at[0] + size] = first
                outs[x][:, at[1] : at[1] + size] = second


def pick(sz, which, notes, clip, own, other):
    c = sz.chips
    group = sz.groups[which]
    return pl.pallas_call(
        functools.partial(pick_kernel, sz, group),
        in_specs=[VMEM] * (2 * c + 2),
        out_specs=[VMEM] * c,
        out_shape=[out(sz.piece, width(group, 2))] * c,
        name="pick",
    )(notes, clip, *own, *other)


def land_kernel(sz, which, notes, *rest):
    c, n = sz.chips, len(which)
    early, late = rest[:n], rest[n : 2 * n]
    outs = rest[2 * n + 3 : 2 * n + 6]
    st, full, sem = rest[2 * n + 6 :]
    n_slots = sz.layers * sz.group
    chip = lax.div(read(notes, n_slots + sz.layers), CORES)
    e, f = sz.early, sz.full
    copies = []
    for j, x in enumerate(which):
        k = dyn_peer(chip, x, c) if c & (c - 1) == 0 else lax.rem(chip - x + c, c)
        a, b = early[j], late[j]
        spot = j if sz.by_piece else k
        first, second = a[:, f : f + e], a[:, f + e : f + 2 * e]
        st[0, spot, :, :e] = new_weights(a[:, :e], first, second)
        st[1, spot, :, :e] = first
        st[2, spot, :, :e] = second
        first, second = b[:, : sz.late], b[:, sz.lat : sz.lat + sz.late]
        st[0, spot, :, e:] = new_weights(a[:, e : sz.cols], first, second)
        st[1, spot, :, e:] = first
        st[2, spot, :, e:] = second
        if sz.by_piece:
            layer = lax.div(k, sz.per_layer)
            row = pl.multiple_of(lax.rem(k, sz.per_layer) * sz.piece, sz.piece)
            slot = read(notes, n_slots + layer)
            for i in range(3):
                there = outs[i].at[layer, slot, pl.ds(row, sz.piece)]
                copies.append(pltpu.make_async_copy(st.at[i, j], there, sem.at[i, j]))
                copies[-1].start()
    if not sz.by_piece:
        for i in range(sz.layers):
            slot = read(notes, n_slots + i)
            for a in range(3):
                for q in range(sz.per_layer):
                    r = slice(q * sz.piece, (q + 1) * sz.piece)
                    full[a, i, r, :] = st[a, i * sz.per_layer + q]
                copies.append(
                    pltpu.make_async_copy(full.at[a, i], outs[a].at[i, slot], sem.at[a, i])
                )
                copies[-1].start()
    for cp in copies:
        cp.wait()


def land(sz, which, notes, early, late, outs):
    f32 = jnp.float32
    n = len(which)
    whole = (8, LANES) if sz.by_piece else (3, sz.layers, sz.rows, sz.cols)
    return pl.pallas_call(
        functools.partial(land_kernel, sz, which),
        in_specs=[VMEM] * (2 * n + 1) + [ANY] * 3,
        out_specs=[ANY] * 3,
        out_shape=[jax.ShapeDtypeStruct(o.shape, o.dtype) for o in outs],
        scratch_shapes=[
            pltpu.VMEM((3, n, sz.piece, sz.cols), f32),
            pltpu.VMEM(whole, f32),
            pltpu.SemaphoreType.DMA((3, max(n, sz.layers))),
        ],
        input_output_aliases={1 + 2 * n + a: a for a in range(3)},
        name="land",
    )(notes, *[early[x] for x in which], *[late[x] for x in which], *outs)


def shifts(sz, arrays):
    c = sz.chips
    got = [arrays[0]] * c
    for x in sz.order:
        pairs = [
            (i * CORES + k, peer(i, x, c) * CORES + k) for i in range(c) for k in range(CORES)
        ]
        got[x] = lax.ppermute(arrays[x], "expert", pairs)
    return got


def spread(sz, arrays):
    return near(shifts(sz, near(arrays)))


def from_others(value, axis):
    n = lax.axis_size(axis)
    return sum(
        lax.ppermute(value, axis, [(i, peer(i, x, n)) for i in range(n)]) for x in range(1, n)
    )


def swap(sz, arrays):
    pairs = [(i, i ^ 1) for i in range(sz.group)]
    return [lax.ppermute(a, "expert", pairs) for a in arrays]


def shards(master, moment_one, moment_two, gradient, old_slot, new_slot):
    sz = Sizes(master.shape, lax.axis_size("expert"), lax.axis_size("dp"))
    me = lax.axis_index("expert").reshape(1)
    c = sz.chips
    got = prep(sz, me, old_slot, new_slot, master, moment_one, moment_two, gradient)
    pieces, raw, total = list(got[:c]), got[c], got[c + 1]
    (notes,) = near([got[c + 2]])
    totals = shifts(sz, [total] * c)
    held = spread(sz, pieces)
    total = sum(totals)
    total = total + swap(sz, [total])[0]
    total = total + from_others(total, "dp")
    clip, clip_copy, *late = scale_and_late(sz, total, raw)
    (clip,) = near([clip])
    late_held = spread(sz, late)
    other = near(swap(sz, held))
    early_out = pick(sz, 0, notes, clip, held, other)
    early_in = spread(sz, list(early_out))
    late_other = near(swap(sz, late_held))
    late_out = pick(sz, 1, notes, clip, late_held, late_other)
    late_in = spread(sz, list(late_out))
    scale = clip_copy[0, 0]
    wide = gradient.astype(jnp.float32)
    first, second = moments(moment_one, moment_two, wide, scale)
    weights = new_weights(master, first, second)
    outs = (weights, first, second)
    half = c // 2
    batches = [range(half), range(half, c)] if sz.by_piece else [range(c)]
    for which in batches:
        outs = land(sz, list(which), notes, early_in, late_in, outs)
    return tuple(outs)


def solution(mesh):
    spec = P(None, "expert", "dp", None)
    return jax.shard_map(
        shards,
        mesh=mesh,
        in_specs=(spec, spec, spec, spec, P(), P()),
        out_specs=(spec, spec, spec),
        check_vma=False,
    )
```

```python
import functools
import math

import jax
import jax.numpy as jnp
from jax import lax
from jax.experimental import pallas as pl
from jax.experimental.pallas import tpu as pltpu
from jax.sharding import PartitionSpec as P


BETA_ONE = 0.9
BETA_TWO = 0.95
LEARN_RATE = 0.05
DECAY_RATE = 0.1
ADAM_EPS = 1e-08
CLIP_RMS = 2.0
FIRST_FIX = 1.0 - 0.9**10
SECOND_FIX = 1.0 - 0.95**10

LANES = 128
CORES = 2
EARLY = 0.18

ANY = pl.BlockSpec(memory_space=pl.ANY)
SMEM = pl.BlockSpec(memory_space=pltpu.SMEM)
VMEM = pl.BlockSpec(memory_space=pltpu.VMEM)


def out(*shape, dtype=jnp.float32):
    return pltpu.VMEM(shape, dtype)


def near(arrays):
    return [pltpu.with_memory_space_constraint(a, pltpu.VMEM) for a in arrays]


def up(n):
    return -(-n // LANES) * LANES


def moments(moment_one, moment_two, gradient, clip_scale):
    scaled = gradient * clip_scale
    first = BETA_ONE * moment_one + (1.0 - BETA_ONE) * scaled
    second = BETA_TWO * moment_two + (1.0 - BETA_TWO) * scaled * scaled
    return first, second


def new_weights(master, first, second):
    step_dir = first / FIRST_FIX / (jnp.sqrt(second / SECOND_FIX) + ADAM_EPS)
    return master - LEARN_RATE * (step_dir + DECAY_RATE * master)


class Sizes:
    def __init__(self, shape, group, dp):
        self.layers, self.slots, self.rows, self.cols = shape
        self.group = group
        self.devices = group * dp
        self.chips = group // CORES
        self.order = [*range(self.chips // 2, self.chips), *range(1, self.chips // 2)]
        self.piece = self.layers * self.rows // self.chips
        self.per_layer = self.rows // self.piece
        self.by_piece = self.piece % 8 == 0
        early = round(self.cols * EARLY / LANES) * LANES
        self.early = early
        self.late = self.cols - early
        self.lat = self.late if self.late % (LANES // 2) == 0 else up(self.late)
        self.full = up(self.cols)
        self.groups = ((self.full, 0, early, early), (0, early, self.late, self.lat))


def width(group, parts):
    head, _, _, stride = group
    return head + parts * stride


def read(note, place):
    lane = lax.broadcasted_iota(jnp.int32, note.shape, 1)
    return jnp.max(jnp.where(lane == place, note[...], 0))


def peer(i, x, n):
    return i ^ x if n & (n - 1) == 0 else (i + x) % n


def dyn_peer(i, x, n):
    return i ^ x if n & (n - 1) == 0 else lax.rem(i + x, n)


def prep_kernel(sz, old_ref, new_ref, master, mone, mtwo, grad, *rest):
    c = sz.chips
    pieces = rest[:c]
    late_raw, total, notes, plan, mv, m1v, m2v, gv, st, sem_g, sem = rest[c:]
    for i in range(sz.layers):
        pltpu.make_async_copy(grad.at[i], gv.at[i], sem_g.at[i]).start()
    me = lax.axis_index("expert")
    chip = lax.div(me, CORES)
    n_slots = sz.layers * sz.group

    for i in range(sz.layers):
        def note(e, carry):
            o = old_ref[i, e]
            n = new_ref[i, e]
            place = jnp.where(o != n, i * sz.group + lax.div(n, sz.slots), n_slots)
            plan[0, place] = lax.div(o, sz.slots)
            plan[1, place] = lax.rem(n, sz.slots)
            return carry

        lax.fori_loop(0, old_ref.shape[1], note, 0, unroll=8)
        slot = plan[1, i * sz.group + me]
        for a, (src, dst) in enumerate(((master, mv), (mone, m1v), (mtwo, m2v))):
            pltpu.make_async_copy(src.at[i, slot], dst.at[i], sem.at[i, a]).start()
    acc = jnp.zeros((sz.rows, sz.cols), jnp.float32)
    for i in range(sz.layers):
        pltpu.make_async_copy(grad.at[i], gv.at[i], sem_g.at[i]).wait()
        for s in range(sz.slots):
            x = gv[i, s].astype(jnp.float32)
            acc = acc + x * x
    total[...] = jnp.broadcast_to(jnp.sum(acc), total.shape)
    for i in range(sz.layers):
        for a, (src, dst) in enumerate(((master, mv), (mone, m1v), (mtwo, m2v))):
            pltpu.make_async_copy(src.at[i, 0], dst.at[i], sem.at[i, a]).wait()
        g = gv[i, plan[1, i * sz.group + me]].astype(jnp.float32)
        for q in range(sz.per_layer):
            k = i * sz.per_layer + q
            r = slice(q * sz.piece, (q + 1) * sz.piece)
            st[0, k] = mv[i, r, :]
            st[1, k] = m1v[i, r, :]
            st[2, k] = m2v[i, r, :]
            st[3, k] = g[r, :]
    lane = lax.broadcasted_iota(jnp.int32, notes.shape, 1)
    table = jnp.where(lane == n_slots + sz.layers, me, 0)
    for i in range(n_slots):
        table = jnp.where(lane == i, plan[0, i], table)
    for i in range(sz.layers):
        table = jnp.where(lane == n_slots + i, plan[1, i * sz.group + me], table)
    notes[...] = table
    for x in range(c):
        k = dyn_peer(chip, x, c)
        pieces[x][:, : sz.cols] = st[0, k]
        for a in range(3):
            lo = sz.full + a * sz.early
            pieces[x][:, lo : lo + sz.early] = st[a + 1, k, :, : sz.early]
            late_raw[a, x] = st[a + 1, k, :, sz.early :]


def prep(sz, old_slot, new_slot, master, mone, mtwo, grad):
    f32 = jnp.float32
    slot = (sz.layers, sz.rows, sz.cols)
    outs = [out(sz.piece, width(sz.groups[0], 3))] * sz.chips + [
        out(3, sz.chips, sz.piece, sz.late),
        out(1, LANES),
        out(1, up(sz.layers * (sz.group + 1) + 1), dtype=jnp.int32),
    ]
    return pl.pallas_call(
        functools.partial(prep_kernel, sz),
        in_specs=[SMEM, SMEM, ANY, ANY, ANY, ANY],
        out_specs=[VMEM] * (sz.chips + 3),
        out_shape=outs,
        scratch_shapes=[
            pltpu.SMEM((2, sz.layers * sz.group + 1), jnp.int32),
            pltpu.VMEM(slot, f32),
            pltpu.VMEM(slot, f32),
            pltpu.VMEM(slot, f32),
            pltpu.VMEM(grad.shape, grad.dtype),
            pltpu.VMEM((4, sz.chips, sz.piece, sz.cols), f32),
            pltpu.SemaphoreType.DMA((sz.layers,)),
            pltpu.SemaphoreType.DMA((sz.layers, 3)),
        ],
        name="prep",
    )(old_slot, new_slot, master, mone, mtwo, grad)


def scale_kernel(sz, total, raw, clip, clip_copy, *late):
    entries = sz.layers * sz.slots * sz.rows * sz.cols * sz.devices
    scale = jnp.minimum(
        1.0, CLIP_RMS * math.sqrt(entries) / (jnp.sqrt(total[...]) + 1e-06)
    )
    clip[...] = scale
    clip_copy[...] = scale
    for x in range(sz.chips):
        first, second = moments(raw[0, x], raw[1, x], raw[2, x], scale[:, 0:1])
        late[x][:, : sz.late] = first
        late[x][:, sz.lat : sz.lat + sz.late] = second


def scale_and_late(sz, total, raw):
    return pl.pallas_call(
        functools.partial(scale_kernel, sz),
        in_specs=[VMEM, VMEM],
        out_specs=[VMEM] * (sz.chips + 2),
        out_shape=[out(1, LANES), jax.ShapeDtypeStruct((1, LANES), jnp.float32)]
        + [out(sz.piece, width(sz.groups[1], 2))] * sz.chips,
        name="scale_late",
    )(*near((total, raw)))


def pick_kernel(sz, group, notes, clip, *rest):
    c = sz.chips
    refs = rest[: 2 * c]
    outs = rest[2 * c : 3 * c]
    head, _, size, stride = group
    at = [head + a * stride for a in range(3)]
    me = lax.axis_index("expert")
    chip = lax.div(me, CORES)
    core = lax.rem(me, CORES)
    layer = lax.div(chip, sz.per_layer)
    for x in range(c):
        target = dyn_peer(chip, x, c) * CORES + core
        sender = read(notes, layer * sz.group + target)
        from_chip = lax.div(sender, CORES)
        shift = from_chip ^ chip if c & (c - 1) == 0 else lax.rem(chip - from_chip + c, c)
        choice = shift + jnp.where(lax.rem(sender, CORES) == core, 0, c)
        for q in range(2 * c):
            @pl.when(choice == q)
            def _():
                if not head:
                    outs[x][...] = refs[q][...]
                    return
                parts = [refs[q][:, lo : lo + size] for lo in at]
                first, second = moments(*parts, clip[:, 0:1])
                outs[x][:, :head] = refs[q][:, :head]
                outs[x][:, at[0] : at[0] + size] = first
                outs[x][:, at[1] : at[1] + size] = second


def pick(sz, which, notes, clip, own, other):
    c = sz.chips
    group = sz.groups[which]
    return pl.pallas_call(
        functools.partial(pick_kernel, sz, group),
        in_specs=[VMEM] * (2 * c + 2),
        out_specs=[VMEM] * c,
        out_shape=[out(sz.piece, width(group, 2))] * c,
        name="pick",
    )(notes, clip, *own, *other)


def land_kernel(sz, which, notes, *rest):
    c, n = sz.chips, len(which)
    early, late = rest[:n], rest[n : 2 * n]
    outs = rest[2 * n + 3 : 2 * n + 6]
    st, full, sem = rest[2 * n + 6 :]
    n_slots = sz.layers * sz.group
    chip = lax.div(lax.axis_index("expert"), CORES)
    e, f = sz.early, sz.full
    copies = []
    for j, x in enumerate(which):
        k = dyn_peer(chip, x, c) if c & (c - 1) == 0 else lax.rem(chip - x + c, c)
        a, b = early[j], late[j]
        spot = j if sz.by_piece else k
        first_e, second_e = a[:, f : f + e], a[:, f + e : f + 2 * e]
        first, second = b[:, : sz.late], b[:, sz.lat : sz.lat + sz.late]
        layer = lax.div(k, sz.per_layer)
        row = pl.multiple_of(lax.rem(k, sz.per_layer) * sz.piece, sz.piece)
        slot = read(notes, n_slots + layer)

        def send(i):
            if sz.by_piece:
                there = outs[i].at[layer, slot, pl.ds(row, sz.piece)]
                copies.append(pltpu.make_async_copy(st.at[i, j], there, sem.at[i, j]))
                copies[-1].start()

        st[1, spot, :, :e] = first_e
        st[1, spot, :, e:] = first
        send(1)
        st[2, spot, :, :e] = second_e
        st[2, spot, :, e:] = second
        send(2)
        st[0, spot, :, :e] = new_weights(a[:, :e], first_e, second_e)
        st[0, spot, :, e:] = new_weights(a[:, e : sz.cols], first, second)
        send(0)
    if not sz.by_piece:
        for i in range(sz.layers):
            slot = read(notes, n_slots + i)
            for a in range(3):
                for q in range(sz.per_layer):
                    r = slice(q * sz.piece, (q + 1) * sz.piece)
                    full[a, i, r, :] = st[a, i * sz.per_layer + q]
                copies.append(
                    pltpu.make_async_copy(full.at[a, i], outs[a].at[i, slot], sem.at[a, i])
                )
                copies[-1].start()
    for cp in copies:
        cp.wait()


def land(sz, which, notes, early, late, outs):
    f32 = jnp.float32
    n = len(which)
    whole = (8, LANES) if sz.by_piece else (3, sz.layers, sz.rows, sz.cols)
    return pl.pallas_call(
        functools.partial(land_kernel, sz, which),
        in_specs=[VMEM] * (2 * n + 1) + [ANY] * 3,
        out_specs=[ANY] * 3,
        out_shape=[jax.ShapeDtypeStruct(o.shape, o.dtype) for o in outs],
        scratch_shapes=[
            pltpu.VMEM((3, n, sz.piece, sz.cols), f32),
            pltpu.VMEM(whole, f32),
            pltpu.SemaphoreType.DMA((3, max(n, sz.layers))),
        ],
        input_output_aliases={1 + 2 * n + a: a for a in range(3)},
        name="land",
    )(notes, *[early[x] for x in which], *[late[x] for x in which], *outs)


def shifts(sz, arrays):
    c = sz.chips
    got = [arrays[0]] * c
    for x in sz.order:
        pairs = [
            (i * CORES + k, peer(i, x, c) * CORES + k) for i in range(c) for k in range(CORES)
        ]
        got[x] = lax.ppermute(arrays[x], "expert", pairs)
    return got


def spread(sz, arrays):
    return near(shifts(sz, near(arrays)))


def from_others(value, axis):
    n = lax.axis_size(axis)
    return sum(
        lax.ppermute(value, axis, [(i, peer(i, x, n)) for i in range(n)]) for x in range(1, n)
    )


def swap(sz, arrays):
    pairs = [(i, i ^ 1) for i in range(sz.group)]
    return [lax.ppermute(a, "expert", pairs) for a in arrays]


def shards(master, moment_one, moment_two, gradient, old_slot, new_slot):
    sz = Sizes(master.shape, lax.axis_size("expert"), lax.axis_size("dp"))
    c = sz.chips
    got = prep(sz, old_slot, new_slot, master, moment_one, moment_two, gradient)
    pieces, raw, total = list(got[:c]), got[c], got[c + 1]
    (notes,) = near([got[c + 2]])
    totals = shifts(sz, [total] * c)
    held = spread(sz, pieces)
    total = sum(totals)
    total = total + swap(sz, [total])[0]
    total = total + from_others(total, "dp")
    clip, clip_copy, *late = scale_and_late(sz, total, raw)
    (clip,) = near([clip])
    late_held = spread(sz, late)
    other = near(swap(sz, held))
    early_out = pick(sz, 0, notes, clip, held, other)
    early_in = spread(sz, list(early_out))
    late_other = near(swap(sz, late_held))
    late_out = pick(sz, 1, notes, clip, late_held, late_other)
    late_in = spread(sz, list(late_out))
    scale = clip_copy[0, 0]
    wide = gradient.astype(jnp.float32)
    first, second = moments(moment_one, moment_two, wide, scale)
    weights = new_weights(master, first, second)
    outs = (weights, first, second)
    half = c // 2
    batches = [range(half), range(half, c)] if sz.by_piece else [range(c)]
    for which in batches:
        outs = land(sz, list(which), notes, early_in, late_in, outs)
    return tuple(outs)


def solution(mesh):
    spec = P(None, "expert", "dp", None)
    return jax.shard_map(
        shards,
        mesh=mesh,
        in_specs=(spec, spec, spec, spec, P(), P()),
        out_specs=(spec, spec, spec),
        check_vma=False,
    )
```
